256 devices in a mesh: tm: 64 (over z, y, x_lo), space: 4 (over x_hi, core).
Axes of the slice: x: 4 (x_hi: 2, x_lo: 2; x = x_hi * 2 + x_lo), y: 4, z: 8, core: 2. Of those that a mesh axis runs over, the one named last changes fastest.
Arguments:
- increments: float32 [64, 3, 512, 1024], P('tm', None, 'space'), may hold values from -6 to 6
- start_state: float32 [3, 512, 1024], P(None, 'space'), may hold values from -6 to 6
- depth: float32 [512, 1024], P('space'), may hold values from 0.5 to 1.5
- error_weight: float32 [3, 512, 1024], P(None, 'space'), may hold values from 0.25 to 1
- obs_index: int32 [64, 4096], P('tm'), may hold values from 0 to 1572863
- obs_count: int32 [64], P('tm'), may hold values from 1024 to 4096, as said below
- obs_value: float32 [64, 4096], P('tm'), may hold values from -6 to 6
- obs_weight: float32 [64, 4096], P('tm'), may hold values from 0.5 to 2
Outputs:
- analysis: float32 [64, 3, 512, 1024], P('tm', None, 'space')
- costs: float32 [2, 64], P(None, 'tm')
The draws below stay inside these ranges and needn't reach their ends.
Inputs may be any that keep to these rules, and one draw needn't show every extreme that they name: Only the first obs_count entries of a subwindow's observation rows are live; some subwindow has all 4096 live.
All inputs are finite; a program needn't handle non-finite values.
Results may differ from the reference program's by a relative error of at most 0.0001.
Values sent between devices are 32-bit elements; how exact they have to be, the bound alone decides.
A program may use at most 128 MiB of HBM per device.

```python
import math
import jax
import jax.numpy as jnp

LON = 1024
NOBS = 4096
STEPS = 6
ITERS = 2
SUBWIN = 64
LAT = 512


def draw_obs_count(key, part):
    first_key, second_key = jax.random.split(jax.random.fold_in(key, 17))
    counted = jax.random.randint(first_key, (SUBWIN,), NOBS // 4, NOBS + 1)
    position = jax.random.randint(second_key, (), 0, SUBWIN)
    return counted.at[position].set(NOBS).astype(jnp.int32)


def touch_ends(entries, own_key, least, top_value):
    longest = entries.shape.index(max(entries.shape))
    spots = []
    for shift in (0, 1):
        where = [jax.random.randint(jax.random.fold_in(own_key, axis), (), 0, length) for axis, length in enumerate(entries.shape)]
        where[longest] = (where[longest] + shift) % entries.shape[longest]
        spots.append(tuple(where))
    return entries.at[spots[0]].set(least).at[spots[1]].set(top_value)


def shard_levels(key, shape, cuts, smallest, largest):
    factor_of, own = 1.0, jax.random.fold_in(key, 6)
    for dim, parts in cuts:
        steps = jnp.exp(jax.random.uniform(jax.random.fold_in(own, dim), (parts,), jnp.float32, smallest / len(cuts), largest / len(cuts)))
        factor_of = factor_of * jnp.repeat(steps, shape[dim] // parts).reshape([-1 if axis == dim else 1 for axis in range(len(shape))])
    return factor_of


def noise(stream_key, dims, width, bound, pieces=(), held_as=jnp.bfloat16):
    drawn = jax.random.normal(stream_key, dims, jnp.float32) * width
    if len(pieces) > 0:
        drawn = shard_levels(stream_key, dims, pieces, -0.22, 0.18) * drawn
    return jnp.clip(drawn, min=-bound, max=bound).astype(held_as)


def setup_inputs(seed: int = 0) -> dict:
    streams_of = jax.random.split(jax.random.key(seed), 9)
    return {
        "increments": noise(streams_of[0], (SUBWIN, 3, LAT, LON), 1.0, 6.0, ((0, 64), (2, 4)), jnp.float32),
        "start_state": noise(streams_of[1], (3, LAT, LON), 1.0, 6.0, ((1, 4),), jnp.float32),
        "depth": jnp.clip(jnp.exp(math.log(1.5) - 1.0986123 * jax.random.uniform(streams_of[2], (LAT, LON), jnp.float32) ** shard_levels(streams_of[2], (LAT, LON), ((0, 4),), -0.2, 0.2)), 0.5, 1.5),
        "error_weight": jnp.clip(jnp.exp(math.log(1.0) - 1.3862944 * jax.random.uniform(streams_of[3], (3, LAT, LON), jnp.float32) ** shard_levels(streams_of[3], (3, LAT, LON), ((1, 4),), -0.2, 0.2)), 0.25, 1.0),
        "obs_index": touch_ends(jax.random.randint(streams_of[4], (SUBWIN, NOBS), 0, 3 * LAT * LON), jax.random.fold_in(streams_of[4], 1), 0, (3 * LAT * LON) - 1).astype(jnp.int32),
        "obs_count": draw_obs_count(jax.random.fold_in(streams_of[8], 71), 0),
        "obs_value": noise(streams_of[6], (SUBWIN, NOBS), 1.0, 6.0, ((0, 64),), jnp.float32),
        "obs_weight": jnp.clip(jnp.exp(math.log(2.0) - 1.3862944 * jax.random.uniform(streams_of[7], (SUBWIN, NOBS), jnp.float32) ** shard_levels(streams_of[7], (SUBWIN, NOBS), ((0, 64),), -0.2, 0.2)), 0.5, 2.0),
    }


COURANT = 0.35
CORIOLIS_MAX = 0.2
STEP_SIZE = 0.2


def coriolis(total_rows, first_row, row_count):
    latitude = ((first_row + jnp.arange(row_count)).astype(jnp.float32) + 0.5) / total_rows * math.pi - math.pi / 2
    return (CORIOLIS_MAX * jnp.sin(latitude))[:, None]


def diff_lon(field):
    return (jnp.roll(field, -1, -1) - jnp.roll(field, 1, -1)) * 0.5


def diff_lat(field):
    widths = [(0, 0)] * (field.ndim - 2) + [(1, 1), (0, 0)]
    padded = jnp.pad(field, widths)
    return (padded[..., 2:, :] - padded[..., :-2, :]) * 0.5


def forward_model(state, depth, rate):
    zonal, merid, height = state[:, 0], state[:, 1], state[:, 2]
    for step in range(STEPS):
        height = height - COURANT * (diff_lon(depth * zonal) + diff_lat(depth * merid))
        zonal = zonal + rate * merid - COURANT * diff_lon(height)
        merid = merid - rate * zonal - COURANT * diff_lat(height)
    return jnp.stack([zonal, merid, height], 1)


def adjoint_model(state, depth, rate):
    adj_zonal, adj_merid, adj_height = state[:, 0], state[:, 1], state[:, 2]
    for step in range(STEPS):
        zonal_mix = adj_zonal - rate * adj_merid
        height_mix = adj_height + COURANT * diff_lat(adj_merid) + COURANT * diff_lon(zonal_mix)
        adj_zonal = zonal_mix + COURANT * depth * diff_lon(height_mix)
        adj_merid = adj_merid + rate * zonal_mix + COURANT * depth * diff_lat(height_mix)
        adj_height = height_mix
    return jnp.stack([adj_zonal, adj_merid, adj_height], 1)


def reference(increments, start_state, depth, error_weight, obs_index, obs_count, obs_value, obs_weight):
    rate = coriolis(LAT, 0, LAT)
    state = increments
    cells = 3 * LAT * LON
    is_live = jnp.arange(NOBS)[None, :] < obs_count[:, None]

    def deposit(where_idx, values):
        return jnp.zeros((cells,), jnp.float32).at[where_idx].add(values)

    cost_list = []
    for sweep_index in range(ITERS):
        endpoints = forward_model(state, depth, rate)
        previous = jnp.concatenate([start_state[None], endpoints[:-1]], 0)
        model_gap = state - previous
        weighted_gap = error_weight * model_gap
        back_image = jnp.concatenate([adjoint_model(weighted_gap[1:], depth, rate), jnp.zeros_like(weighted_gap[:1])], 0)
        flattened = state.reshape(state.shape[0], -1)
        observed = jnp.take_along_axis(flattened, obs_index, 1)
        resid = jnp.where(is_live, observed - obs_value, 0.0)
        weighted = obs_weight * resid
        obs_grad = jax.vmap(deposit)(obs_index, weighted).reshape(state.shape)
        cost_now = (0.5 * jnp.sum(weighted_gap * model_gap, (1, 2, 3)) + 0.5 * jnp.sum(weighted * resid, 1)) / cells
        cost_list.append(cost_now)
        state = state - STEP_SIZE * (weighted_gap - back_image + obs_grad)
    return state, jnp.stack(cost_list, 0)
```

```python
import functools
import math

import jax
import jax.numpy as jnp
from jax import lax
from jax.experimental import pallas as pl
from jax.experimental.pallas import tpu as pltpu
from jax.sharding import PartitionSpec as P

STEPS = 6
ITERS = 2
COURANT = 0.35
HALF = 0.5 * COURANT
CORIOLIS_MAX = 0.2
STEP_SIZE = 0.2
HALO = 2 * STEPS
TOP = 16
BLK = 8
STREAMS = 4
ORDER = (0, 3, 1, 2)
MESH = pl.DeviceIdType.MESH


def dlon(f):
    lane = lax.broadcasted_iota(jnp.int32, f.shape, 2)
    g = pltpu.roll(f, 127, axis=2)
    g = jnp.where(lane == 127, pltpu.roll(g, 7, axis=1), g)
    m = pltpu.roll(f, 1, axis=2)
    m = jnp.where(lane == 0, pltpu.roll(m, 1, axis=1), m)
    return g - m


def row_blocks(rows):
    low, high = TOP - HALO, TOP + rows + HALO
    return [(r, min(BLK, high - r)) for r in range(low, high, BLK)]


def edge_rows(T, rows, keep_top, keep_bottom):
    T[2, TOP - 1] = T[2, TOP - 1] * keep_top
    T[2, TOP + rows] = T[2, TOP + rows] * keep_bottom


def forward(T, D, F, rows, keep_top, keep_bottom):
    def step(_, carry):
        for r, n in row_blocks(rows):
            du = D[r : r + n] * T[0, r : r + n]
            above = D[r + 1 : r + 1 + n] * T[1, r + 1 : r + 1 + n]
            below = D[r - 1 : r - 1 + n] * T[1, r - 1 : r - 1 + n]
            T[2, r : r + n] = T[2, r : r + n] - (dlon(du) + (above - below))
        edge_rows(T, rows, keep_top, keep_bottom)
        for r, n in row_blocks(rows):
            f = F[r : r + n]
            v = T[1, r : r + n]
            u = T[0, r : r + n] + f * v - HALF * dlon(T[2, r : r + n])
            T[0, r : r + n] = u
            T[1, r : r + n] = v - f * u - HALF * (T[2, r + 1 : r + 1 + n] - T[2, r - 1 : r - 1 + n])
        return carry

    lax.fori_loop(0, STEPS, step, 0)


def adjoint(T, D, F, rows, keep_top, keep_bottom):
    def step(_, carry):
        for r, n in row_blocks(rows):
            a = T[0, r : r + n] - F[r : r + n] * T[1, r : r + n]
            T[0, r : r + n] = a
            T[2, r : r + n] = T[2, r : r + n] + HALF * (
                (T[1, r + 1 : r + 1 + n] - T[1, r - 1 : r - 1 + n]) + dlon(a)
            )
        edge_rows(T, rows, keep_top, keep_bottom)
        for r, n in row_blocks(rows):
            a = T[0, r : r + n]
            d = D[r : r + n]
            T[0, r : r + n] = a + d * dlon(T[2, r : r + n])
            T[1, r : r + n] = (
                T[1, r : r + n]
                + F[r : r + n] * a
                + d * (T[2, r + 1 : r + 1 + n] - T[2, r - 1 : r - 1 + n])
            )
        return carry

    lax.fori_loop(0, STEPS, step, 0)


def deposit_kernel(count, code_ref, w_ref, wy_ref, out_w, out_wy, *more):
    grids = [(out_w, out_wy)] + [(more[2 * i], more[2 * i + 1]) for i in range(STREAMS - 1)]
    total = out_w.shape[0]
    zero = jnp.zeros((64, 128), jnp.float32)

    def clear(i, carry):
        at = pl.ds(pl.multiple_of(i * 64, 64), 64)
        for gw, gy in grids:
            gw[at, :] = zero
            gy[at, :] = zero
        return carry

    lax.fori_loop(0, total // 64, clear, 0)
    lanes = lax.broadcasted_iota(jnp.int32, (1, 128), 1)

    def add(i, carry):
        for s, (gw, gy) in enumerate(grids):
            j = i * STREAMS + s
            code = code_ref[j]
            at = pl.ds(code // 128, 1)
            hit = lanes == code % 128
            gw[at, :] = gw[at, :] + jnp.where(hit, w_ref[j], 0.0)
            gy[at, :] = gy[at, :] + jnp.where(hit, wy_ref[j], 0.0)
        return carry

    lax.fori_loop(0, count // STREAMS, add, 0)

    def gather(i, carry):
        at = pl.ds(pl.multiple_of(i * 64, 64), 64)
        out_w[at, :] = sum([g[0][at, :] for g in grids[1:]], out_w[at, :])
        out_wy[at, :] = sum([g[1][at, :] for g in grids[1:]], out_wy[at, :])
        return carry

    lax.fori_loop(0, total // 64, gather, 0)


def place():
    tm, sp = lax.axis_index("tm"), lax.axis_index("space")
    a, y, b, c = tm % 2, tm // 2, sp // 2, sp % 2
    return tm, sp, a, y, b, c, 2 * b + a, 2 * y + c


def main_kernel(
    rows, cells, pairs, bands,
    x_own, x_got, e_hbm, d_hbm, s_hbm, w_hbm, wy_hbm, f_hbm, c0_ref,
    out_hbm, cost_ref,
    stg_x, stg_e, stg_d, stg_s, X, T, A, D, F, E, W, WY, XN, EN, FIN, OUT, cbuf, crecv,
    load_sem, push_send, push_recv, halo_send, halo_recv,
    x_send, x_recv, e_send, e_recv, fin_send, fin_recv, c_send, c_recv, out_sem,
):
    tm, sp, a, y, b, c, band, window = place()
    last = 2 * pairs - 1
    own = a == c
    partner = (tm, 2 * b + (1 - c))
    swap = (2 * y + (1 - a), 2 * b + (1 - c))
    up_band, down_band = lax.rem(band + bands - 1, bands), lax.rem(band + 1, bands)
    up = (2 * y + up_band % 2, 2 * (up_band // 2) + c)
    down = (2 * y + down_band % 2, 2 * (down_band // 2) + c)
    succ_y = lax.rem(y + c, pairs)
    succ = (2 * succ_y + a, 2 * b + (1 - c))
    pred_y = lax.rem(y + pairs - (1 - c), pairs)
    pred = (2 * pred_y + a, 2 * b + (1 - c))
    not_top, not_bottom = band > 0, band < bands - 1
    not_first, not_last = window > 0, window < last
    keep_top = jnp.where(not_top, 1.0, 0.0).astype(jnp.float32)
    keep_bottom = jnp.where(not_bottom, 1.0, 0.0).astype(jnp.float32)
    chunk = rows // len(ORDER)
    inner = pl.ds(TOP, rows)

    loads = [
        pltpu.make_async_copy(src, dst, load_sem.at[i])
        for i, (src, dst) in enumerate(((w_hbm, W), (wy_hbm, WY), (f_hbm, F)))
    ]
    for load in loads:
        load.start()
    load_own = pltpu.make_async_copy(x_own, stg_x, load_sem.at[3])
    load_got = pltpu.make_async_copy(x_got, stg_x, load_sem.at[3])
    load_e = pltpu.make_async_copy(e_hbm, stg_e, load_sem.at[4])
    load_d = pltpu.make_async_copy(d_hbm, stg_d, load_sem.at[5])
    load_s = pltpu.make_async_copy(s_hbm, stg_s, load_sem.at[6])

    @pl.when(own)
    def _():
        load_own.start()
        load_e.start()
        load_d.start()

    @pl.when(jnp.logical_not(own))
    def _():
        load_got.start()

    own_start = own & (y == 0) & (c == 0)
    push_start = own & (y == 0) & (c == 1)
    need_start = jnp.logical_not(own) & (y == 0) & (c == 0)

    @pl.when(own_start)
    def _():
        load_s.start()

    zeros = jnp.zeros((TOP, 8, 128), jnp.float32)
    for buf in (X, A):
        for i in range(3):
            buf[i, 0:TOP] = zeros
            buf[i, TOP + rows : 2 * TOP + rows] = zeros
    D[0:TOP] = zeros
    D[TOP + rows : 2 * TOP + rows] = zeros

    barrier = pltpu.get_barrier_semaphore()
    for da in range(2):
        for s in range(bands):
            other = jnp.logical_not((a == da) & (sp == s))

            @pl.when(other)
            def _(da=da, s=s):
                pl.semaphore_signal(barrier, inc=1, device_id=(2 * y + da, s), device_id_type=MESH)

    far = jnp.where(c == 1, not_last, not_first)
    far_y = jnp.where(c == 1, succ_y, pred_y)

    @pl.when(far)
    def _():
        pl.semaphore_signal(
            barrier, inc=1, device_id=(2 * far_y + a, 2 * b + (1 - c)), device_id_type=MESH
        )

    pl.semaphore_wait(barrier, 2 * bands - 1 + far.astype(jnp.int32))

    def remote(src, dst, send, recv, to):
        return pltpu.make_async_remote_copy(
            src_ref=src, dst_ref=dst, send_sem=send, recv_sem=recv, device_id=to, device_id_type=MESH
        )

    push_e = remote(e_hbm, stg_e, push_send.at[0], push_recv.at[0], partner)
    push_d = remote(d_hbm, stg_d, push_send.at[1], push_recv.at[1], partner)
    push_s = remote(s_hbm, stg_s, push_send.at[2], push_recv.at[2], partner)

    @pl.when(own)
    def _():
        push_d.start()
        push_e.start()

    @pl.when(push_start)
    def _():
        push_s.start()

    def to_rows(stage, store, count):
        def body(i, carry):
            for j in range(8):
                store(i * 8 + j, stage[pl.ds(i * 64 + j, 8, stride=8), :])
            return carry

        lax.fori_loop(0, count // 8, body, 0)

    def three(stage, buf, top):
        def body(i, carry):
            for comp in range(3):
                for j in range(8):
                    buf[comp, top + i * 8 + j] = stage[
                        pl.ds(comp * rows * 8 + i * 64 + j, 8, stride=8), :
                    ]
            return carry

        lax.fori_loop(0, rows // 8, body, 0)

    load_own.wait()
    three(stg_x, X, TOP)

    def chunk_copy(src, src_top, dst, dst_top, j, send, recv, to):
        return remote(
            src.at[:, pl.ds(src_top + j * chunk, chunk)],
            dst.at[:, pl.ds(dst_top + j * chunk, chunk)],
            send,
            recv,
            to,
        )

    def x_copy(it, j):
        return chunk_copy(X, TOP, XN.at[it], 0, j, x_send.at[it, j], x_recv.at[it, j], pred)

    def e_copy(it, j):
        return chunk_copy(T, TOP, EN.at[it], 0, j, e_send.at[it, j], e_recv.at[it, j], succ)

    def fin_copy(j):
        return chunk_copy(X, TOP, FIN, 0, j, fin_send.at[j], fin_recv.at[j], swap)

    def halo_copies(view, h):
        return (
            remote(
                view(TOP), view(TOP + rows), halo_send.at[h, 0], halo_recv.at[h, 0], up
            ),
            remote(
                view(TOP + rows - HALO), view(TOP - HALO), halo_send.at[h, 1], halo_recv.at[h, 1], down
            ),
        )

    def start_halo(view, h):
        to_up, to_down = halo_copies(view, h)

        @pl.when(not_top)
        def _():
            to_up.start()

        @pl.when(not_bottom)
        def _():
            to_down.start()

    def wait_halo(view, h):
        to_up, to_down = halo_copies(view, h)

        @pl.when(not_top)
        def _():
            to_up.wait_send()
            to_down.wait_recv()

        @pl.when(not_bottom)
        def _():
            to_down.wait_send()
            to_up.wait_recv()

    def view_x(r):
        return X.at[:, pl.ds(r, HALO)]

    def view_a(r):
        return A.at[:, pl.ds(r, HALO)]

    def view_d(r):
        return D.at[pl.ds(r, HALO)]

    @pl.when(not_first)
    def _():
        for j in ORDER:
            x_copy(0, j).start()

    start_halo(view_x, 0)

    @pl.when(own)
    def _():
        load_d.wait()

    @pl.when(jnp.logical_not(own))
    def _():
        push_d.wait_recv()

    def store_d(r, value):
        D[TOP + r] = HALF * value

    to_rows(stg_d, store_d, rows)
    start_halo(view_d, 4)

    @pl.when(own)
    def _():
        load_e.wait()
        push_d.wait_send()
        push_e.wait_send()

    @pl.when(jnp.logical_not(own))
    def _():
        push_e.wait_recv()

    three(stg_e, E, 0)

    @pl.when(own_start)
    def _():
        load_s.wait()

    @pl.when(push_start)
    def _():
        push_s.wait_send()

    @pl.when(need_start)
    def _():
        push_s.wait_recv()

    @pl.when(window == 0)
    def _():
        three(stg_s, EN.at[0], 0)
        three(stg_s, EN.at[1], 0)

    for load in loads:
        load.wait()
    wait_halo(view_d, 4)

    for it in range(ITERS):
        final = it == ITERS - 1
        wait_halo(view_x, it)

        def take(i, carry):
            for comp in range(3):
                at = pl.ds(TOP - HALO + i * 8, 8)
                T[comp, at] = X[comp, at]
            return carry

        lax.fori_loop(0, (rows + 2 * HALO) // 8, take, 0)
        forward(T, D, F, rows, keep_top, keep_bottom)

        @pl.when(not_last)
        def _():
            for j in ORDER:
                e_copy(it, j).start()

        for n, j in enumerate(ORDER):

            @pl.when(not_last)
            def _():
                x_copy(it, j).wait_recv()

            def differ(i, carry):
                at = pl.ds(j * chunk + i * 4, 4)
                wide = pl.ds(TOP + j * chunk + i * 4, 4)
                for comp in range(3):
                    value = E[comp, at] * (XN[it, comp, at] - T[comp, wide])
                    A[comp, wide] = jnp.where(not_last, value, 0.0)
                return carry

            lax.fori_loop(0, chunk // 4, differ, 0)
            if n == 1:
                start_halo(view_a, 2 + it)

        wait_halo(view_a, 2 + it)
        adjoint(A, D, F, rows, keep_top, keep_bottom)

        acc = 0.5 * c0_ref[...]
        for n, j in enumerate(ORDER):

            @pl.when(not_first)
            def _():
                x_copy(it, j).wait_send()
                e_copy(it, j).wait_recv()

            def update(i, acc):
                at = pl.ds(j * chunk + i * 4, 4)
                wide = pl.ds(TOP + j * chunk + i * 4, 4)
                for comp in range(3):
                    x = X[comp, wide]
                    gap = x - EN[it, comp, at]
                    lam = E[comp, at] * gap
                    wy = WY[comp, at]
                    grad = W[comp, at] * x - wy
                    acc = acc + 0.5 * jnp.sum(lam * gap + x * (grad - wy), axis=0)
                    X[comp, wide] = x - STEP_SIZE * (lam - A[comp, wide] + grad)
                return acc

            acc = lax.fori_loop(0, chunk // 4, update, acc)
            if final:

                @pl.when(jnp.logical_not(own))
                def _():
                    fin_copy(j).start()

            else:

                @pl.when(not_first)
                def _():
                    x_copy(it + 1, j).start()

                if n == 1:
                    start_halo(view_x, it + 1)

        cbuf[it] = acc

        @pl.when(not_last)
        def _():
            for j in ORDER:
                e_copy(it, j).wait_send()

    def c_copy(s):
        return remote(cbuf, crecv.at[band], c_send.at[s], c_recv.at[band], (2 * y + c, s))

    for s in range(bands):

        @pl.when(jnp.logical_not(own & (sp == s)))
        def _(s=s):
            c_copy(s).start()

    @pl.when(own)
    def _():
        crecv[band] = cbuf[...]

    def out_copy(comp, j):
        at = pl.ds((comp * rows + j * chunk) * 8, chunk * 8)
        return pltpu.make_async_copy(OUT.at[at], out_hbm.at[at], out_sem.at[comp, j])

    def put(src, top, j):
        def body(i, carry):
            for comp in range(3):
                for r in range(8):
                    at = pl.ds(comp * rows * 8 + j * chunk * 8 + i * 64 + r, 8, stride=8)
                    OUT[at, :] = src[comp, top + j * chunk + i * 8 + r]
            return carry

        lax.fori_loop(0, chunk // 8, body, 0)

    for j in ORDER:

        @pl.when(own)
        def _():
            put(X, TOP, j)

        @pl.when(jnp.logical_not(own))
        def _():
            fin_copy(j).wait_recv()
            put(FIN, 0, j)

        for comp in range(3):
            out_copy(comp, j).start()

    for s in range(bands):

        @pl.when(jnp.logical_not(own & (sp == s)))
        def _(s=s):
            c_copy(s).wait_send()

        @pl.when(jnp.logical_not(own & (band == s)))
        def _(s=s):
            remote(cbuf, crecv.at[s], c_send.at[s], c_recv.at[s], partner).wait_recv()

    total = crecv[0]
    for s in range(1, bands):
        total = total + crecv[s]
    for it in range(ITERS):
        cost_ref[it, 0] = jnp.sum(total[it]) / cells

    @pl.when(jnp.logical_not(own))
    def _():
        for j in ORDER:
            fin_copy(j).wait_send()

    for j in ORDER:
        for comp in range(3):
            out_copy(comp, j).wait()


def as_tiles(x):
    x = x.reshape(-1, 8, x.shape[-1] // 128, 128)
    return x.transpose(0, 2, 1, 3).reshape(-1, 128)


def from_tiles(x, shape):
    x = x.reshape(-1, shape[-1] // 128, 8, 128)
    return x.transpose(0, 2, 1, 3).reshape(shape)


def per_device(
    increments, start_state, depth, error_weight, obs_index, obs_count, obs_value, obs_weight
):
    rows, columns = increments.shape[2:]
    slots = obs_index.shape[1]
    bands, windows = lax.axis_size("space"), lax.axis_size("tm")
    pairs = windows // 2
    total_rows = rows * bands
    cells = 3 * total_rows * columns
    _, _, a, y, b, c, band, _ = place()
    own = a == c

    exchange = []
    for py in range(pairs):
        for pb in range(bands // 2):
            one = 2 * py * bands + 2 * pb + 1
            two = (2 * py + 1) * bands + 2 * pb
            exchange += [(one, two), (two, one)]
    both = ("tm", "space")

    live = jnp.arange(slots) < obs_count[0]
    packed = jnp.stack(
        [obs_index[0].astype(jnp.float32), jnp.where(live, obs_weight[0], 0.0), obs_value[0]]
    )
    packed_got = lax.ppermute(packed, both, exchange)
    x_got = lax.ppermute(increments, both, exchange)
    packed = jnp.where(own, packed, packed_got)

    index = packed[0].astype(jnp.int32)
    component = index // (total_rows * columns)
    line = index // columns % total_rows - band * rows
    inside = (line >= 0) & (line < rows)
    code = (component * rows + jnp.clip(line, 0, rows - 1)) * columns + index % columns
    weight = jnp.where(inside, packed[1], 0.0)
    weighted = weight * packed[2]
    c0 = jnp.sum((weighted * packed[2]).reshape(-1, 8, 128), 0)

    lines = 3 * rows * 8
    smem = pl.BlockSpec(memory_space=pltpu.SMEM)
    vmem = pl.BlockSpec(memory_space=pltpu.VMEM)
    hbm = pl.BlockSpec(memory_space=pl.ANY)
    grid_type = jax.ShapeDtypeStruct((lines, 128), jnp.float32)
    grid_w, grid_wy = pl.pallas_call(
        functools.partial(deposit_kernel, slots),
        out_shape=(grid_type, grid_type),
        in_specs=[smem] * 3,
        out_specs=(vmem, vmem),
        scratch_shapes=[pltpu.VMEM((lines, 128), jnp.float32)] * (2 * STREAMS - 2),
        cost_estimate=pl.CostEstimate(flops=10**7, bytes_accessed=4 * 10**7, transcendentals=0),
        name="deposit",
    )(code, weight, weighted)

    wide = rows + 2 * TOP
    latitude = ((band * rows - TOP + jnp.arange(wide)).astype(jnp.float32) + 0.5) / total_rows
    rate = CORIOLIS_MAX * jnp.sin(latitude * math.pi - math.pi / 2)
    rate = jnp.broadcast_to(rate[:, None, None], (wide, 8, 128))

    def rows_of(count, lead=(3,)):
        return pltpu.VMEM((*lead, count, 8, 128), jnp.float32)

    tiles = pltpu.VMEM((lines, 128), jnp.float32)
    dma = pltpu.SemaphoreType.DMA
    chunks = len(ORDER)
    out, costs = pl.pallas_call(
        functools.partial(main_kernel, rows, cells, pairs, bands),
        out_shape=(grid_type, jax.ShapeDtypeStruct((ITERS, 1), jnp.float32)),
        in_specs=[hbm] * 8 + [vmem],
        out_specs=(hbm, smem),
        scratch_shapes=[
            tiles, tiles, pltpu.VMEM((rows * 8, 128), jnp.float32), tiles,
            rows_of(wide), rows_of(wide), rows_of(wide),
            rows_of(wide, ()), rows_of(wide, ()),
            rows_of(rows), rows_of(rows), rows_of(rows),
            rows_of(rows, (ITERS, 3)), rows_of(rows, (ITERS, 3)), rows_of(rows), tiles,
            pltpu.VMEM((ITERS, 8, 128), jnp.float32), pltpu.VMEM((bands, ITERS, 8, 128), jnp.float32),
            dma((7,)), dma((3,)), dma((3,)), dma((5, 2)), dma((5, 2)),
            dma((ITERS, chunks)), dma((ITERS, chunks)), dma((ITERS, chunks)), dma((ITERS, chunks)),
            dma((chunks,)), dma((chunks,)), dma((bands,)), dma((bands,)), dma((3, chunks)),
        ],
        compiler_params=pltpu.CompilerParams(
            collective_id=0, has_side_effects=True, vmem_limit_bytes=56 * 2**20
        ),
        name="iterations",
    )(
        as_tiles(increments), as_tiles(x_got), as_tiles(error_weight), as_tiles(depth),
        as_tiles(start_state), grid_w.reshape(3, rows, 8, 128), grid_wy.reshape(3, rows, 8, 128),
        rate, c0,
    )
    return from_tiles(out, increments.shape), costs


def solution(mesh):
    placed = (
        P("tm", None, "space", None),
        P(None, "space", None),
        P("space", None),
        P(None, "space", None),
        P("tm", None),
        P("tm"),
        P("tm", None),
        P("tm", None),
    )
    return jax.shard_map(
        per_device,
        mesh=mesh,
        in_specs=placed,
        out_specs=(P("tm", None, "space", None), P(None, "tm")),
        check_vma=False,
    )
```

```python
import functools
import math

import jax
import jax.numpy as jnp
from jax import lax
from jax.experimental import pallas as pl
from jax.experimental.pallas import tpu as pltpu
from jax.sharding import PartitionSpec as P

STEPS = 6
ITERS = 2
COURANT = 0.35
HALF = 0.5 * COURANT
CORIOLIS_MAX = 0.2
STEP_SIZE = 0.2
HALO = 2 * STEPS
TOP = 24
BLK = 8
STREAMS = 2
UNROLL = 16
VMEM = 36
SCHEDULE = (
    "A00", "U00", "A01", "U01", "A02", "U02", "F10", "E10", "F11",
    "A03", "U03", "F12", "F13", "A10", "U10", "A11", "U11", "A12",
    "U12", "F14", "E11", "A13", "U13", "A14", "U14",
)
MESH = pl.DeviceIdType.MESH


def dlon(f):
    lane = lax.broadcasted_iota(jnp.int32, f.shape, 2)
    g = pltpu.roll(f, 127, axis=2)
    g = jnp.where(lane == 127, pltpu.roll(g, 7, axis=1), g)
    m = pltpu.roll(f, 1, axis=2)
    m = jnp.where(lane == 0, pltpu.roll(m, 1, axis=1), m)
    return g - m


def slab(T, low, high, first, second, edge):
    for s in range(STEPS):
        for r in range(low, high, BLK):
            first(r - 1 - 2 * s, min(BLK, high - r))
        if edge is not None:
            T[2, TOP - 1] = T[2, TOP - 1] * edge
        for r in range(low, high, BLK):
            second(r - 2 - 2 * s, min(BLK, high - r))


def forward(T, D, F, low, high, edge):
    def first(r, n):
        at = pl.ds(r, n)
        above, below = pl.ds(r + 1, n), pl.ds(r - 1, n)
        du = D[at] * T[0, at]
        T[2, at] = T[2, at] - (dlon(du) + (D[above] * T[1, above] - D[below] * T[1, below]))

    def second(r, n):
        at = pl.ds(r, n)
        f = F[at]
        v = T[1, at]
        u = T[0, at] + f * v - HALF * dlon(T[2, at])
        T[0, at] = u
        T[1, at] = v - f * u - HALF * (T[2, pl.ds(r + 1, n)] - T[2, pl.ds(r - 1, n)])

    slab(T, low, high, first, second, edge)


def adjoint(T, D, F, low, high, edge):
    def first(r, n):
        at = pl.ds(r, n)
        a = T[0, at] - F[at] * T[1, at]
        T[0, at] = a
        T[2, at] = T[2, at] + HALF * ((T[1, pl.ds(r + 1, n)] - T[1, pl.ds(r - 1, n)]) + dlon(a))

    def second(r, n):
        at = pl.ds(r, n)
        a = T[0, at]
        d = D[at]
        T[0, at] = a + d * dlon(T[2, at])
        T[1, at] = T[1, at] + F[at] * a + d * (T[2, pl.ds(r + 1, n)] - T[2, pl.ds(r - 1, n)])

    slab(T, low, high, first, second, edge)


def deposit_kernel(count, code_ref, w_ref, wy_ref, out_w, out_wy, *more):
    grids = [(out_w, out_wy)] + [(more[2 * i], more[2 * i + 1]) for i in range(STREAMS - 1)]
    total = out_w.shape[0]
    zero = jnp.zeros((64, 128), jnp.float32)

    def clear(i, carry):
        at = pl.ds(pl.multiple_of(i * 64, 64), 64)
        for gw, gy in grids:
            gw[at, :] = zero
            gy[at, :] = zero
        return carry

    lax.fori_loop(0, total // 64, clear, 0)
    lanes = lax.broadcasted_iota(jnp.int32, (1, 128), 1)

    def add(i, carry):
        for k in range(UNROLL):
            for s, (gw, gy) in enumerate(grids):
                j = (i * UNROLL + k) * STREAMS + s
                code = code_ref[j]
                at = pl.ds(lax.shift_right_logical(code, 7), 1)
                hit = lanes == (code & 127)
                gw[at, :] = gw[at, :] + jnp.where(hit, w_ref[j], 0.0)
                gy[at, :] = gy[at, :] + jnp.where(hit, wy_ref[j], 0.0)
        return carry

    lax.fori_loop(0, count // (STREAMS * UNROLL), add, 0)

    def gather(i, carry):
        at = pl.ds(pl.multiple_of(i * 64, 64), 64)
        out_w[at, :] = sum([g[0][at, :] for g in grids[1:]], out_w[at, :])
        out_wy[at, :] = sum([g[1][at, :] for g in grids[1:]], out_wy[at, :])
        return carry

    lax.fori_loop(0, total // 64, gather, 0)


def place():
    tm, sp = lax.axis_index("tm"), lax.axis_index("space")
    a, y, b, c = tm % 2, tm // 2, sp // 2, sp % 2
    return tm, sp, a, y, b, c, 2 * b + a, 2 * y + c


def limits(rows):
    forward_high = [rows * 3 // 8, rows * 5 // 8, rows * 7 // 8, rows + HALO]
    plan = []
    for _ in range(ITERS):
        e = [r - HALO for r in forward_high]
        adjoint_high = e[:-1] + [rows + HALO]
        u = [r - HALO for r in adjoint_high]
        plan.append((forward_high, e, adjoint_high, u))
        forward_high = u + [rows + HALO]
    return plan


def sent_pieces(rows):
    edge = rows - HALO
    plan = limits(rows)
    x, later = plan[0][0], plan[0][3]
    first = [(0, HALO), (edge, rows), (HALO, x[0])] + list(zip(x[:-2], x[1:-1])) + [(x[-2], edge)]
    then = list(zip([0] + later[:-2], later[:-1])) + [(edge, rows), (later[-2], edge)]
    return first, then


def main_kernel(
    rows, cells, pairs, bands,
    x_own, x_got, e_own, d_own, s_own, W, WY, F, c0_ref,
    OUT, cost_ref,
    stg_e, stg_d, stg_s, X, T, A, D, E, XN, EN, FIN, cbuf, crecv,
    edge_out, edge_in, d_top, d_bottom,
    push_send, push_recv, halo_send, halo_recv,
    x_send, x_recv, e_send, e_recv, fin_send, fin_recv, c_send, c_recv,
):
    tm, sp, a, y, b, c, band, window = place()
    last = 2 * pairs - 1
    own = a == c
    partner = (tm, 2 * b + (1 - c))
    swap = (2 * y + (1 - a), 2 * b + (1 - c))
    flip = a == 1
    sign = jnp.where(flip, -1.0, 1.0).astype(jnp.float32)
    bottom_peer = (2 * y + (1 - a), sp)
    top_band = jnp.where(flip, band + 1, band - 1)
    has_top = (top_band >= 0) & (top_band < bands)
    top_band = lax.rem(top_band + bands, bands)
    top_peer = (2 * y + top_band % 2, 2 * (top_band // 2) + c)
    succ_y = lax.rem(y + c, pairs)
    succ = (2 * succ_y + a, 2 * b + (1 - c))
    pred_y = lax.rem(y + pairs - (1 - c), pairs)
    pred = (2 * pred_y + a, 2 * b + (1 - c))
    not_first, not_last = window > 0, window < last
    edge = jnp.where(has_top, 1.0, 0.0).astype(jnp.float32)
    plan = limits(rows)
    pieces = sent_pieces(rows)

    edge_lines = pl.ds(pl.multiple_of(jnp.where(flip, rows * 8 - 128, 0), 128), 128)
    own_start = own & (y == 0) & (c == 0)
    push_start = own & (y == 0) & (c == 1)
    need_start = jnp.logical_not(own) & (y == 0) & (c == 0)

    barrier = pltpu.get_barrier_semaphore()
    for da in range(2):
        for s in range(bands):
            other = jnp.logical_not((a == da) & (sp == s))

            @pl.when(other)
            def _(da=da, s=s):
                pl.semaphore_signal(barrier, inc=1, device_id=(2 * y + da, s), device_id_type=MESH)

    far = jnp.where(c == 1, not_last, not_first)
    far_y = jnp.where(c == 1, succ_y, pred_y)

    @pl.when(far)
    def _():
        pl.semaphore_signal(
            barrier, inc=1, device_id=(2 * far_y + a, 2 * b + (1 - c)), device_id_type=MESH
        )

    zeros = jnp.zeros((TOP, 8, 128), jnp.float32)
    D[0:TOP] = zeros
    for it in range(ITERS):
        for i in range(3):
            T[it, i, 0:TOP] = zeros
            A[it, i, 0:TOP] = zeros

    def blocks(low, high, size, body, init=0):
        return lax.fori_loop(
            0, (high - low) // size, lambda i, carry: body(low + i * size, carry), init
        )

    def line_of(comp, r, j):
        line = jnp.where(flip, (rows - 8 - r) * 8 + 7 - j, r * 8 + j)
        return pl.ds(comp * rows * 8 + line, 8, stride=8)

    def each_row(stage, comps, store):
        def body(r, carry):
            for comp in range(comps):
                for j in range(8):
                    store(comp, r + j, stage[line_of(comp, r, j), :])
            return carry

        blocks(0, rows, 8, body)

    def store_x(comp, r, value):
        if comp == 1:
            value = value * sign
        X[comp, r] = value
        T[0, comp, TOP + r] = value

    @pl.when(own)
    def _():
        each_row(x_own, 3, store_x)

    @pl.when(jnp.logical_not(own))
    def _():
        each_row(x_got, 3, store_x)

    pl.semaphore_wait(barrier, 2 * bands - 1 + far.astype(jnp.int32))

    def remote(src, dst, send, recv, to):
        return pltpu.make_async_remote_copy(
            src_ref=src, dst_ref=dst, send_sem=send, recv_sem=recv, device_id=to, device_id_type=MESH
        )

    push_e = remote(e_own, stg_e, push_send.at[0], push_recv.at[0], partner)
    push_d = remote(d_own, stg_d, push_send.at[1], push_recv.at[1], partner)
    push_s = remote(s_own, stg_s, push_send.at[2], push_recv.at[2], partner)

    push_bottom = remote(d_own.at[edge_lines], d_bottom, push_send.at[3], push_recv.at[3], partner)
    push_top = [
        remote(
            d_own.at[edge_lines], d_top, push_send.at[4 + i], push_recv.at[4], (top_peer[0], 2 * (top_band // 2) + i)
        )
        for i in range(2)
    ]

    @pl.when(own)
    def _():
        push_d.start()
        pl.when(has_top)(lambda: [push.start() for push in push_top] and None)

    @pl.when(jnp.logical_not(own))
    def _():
        push_bottom.start()

    @pl.when(push_start)
    def _():
        push_s.start()

    def piece(ref, low, high, top):
        return ref.at[:, pl.ds(top + low, high - low)]

    def span(ends, j):
        return (ends[j - 1] if j else 0), ends[j]

    def x_copy(it, i):
        low, high = pieces[it][i]
        return remote(
            piece(X, low, high, 0), piece(XN.at[it], low, high, 0), x_send.at[it, i], x_recv.at[it, i], pred
        )

    arrived, sent, late = set(), set(), {}

    def some(done, it, low, high):
        fresh = [i for i, (p, q) in enumerate(pieces[it]) if p < high and q > low and (it, i) not in done]
        done.update((it, i) for i in fresh)
        return fresh

    def need_x(it, low, high):
        fresh = some(arrived, it, low, high)

        @pl.when(not_last)
        def _():
            for i in fresh:
                x_copy(it, i).wait_recv()

    def need_sent(it, low, high):
        fresh = some(sent, it, low, high)

        @pl.when(not_first)
        def _():
            for i in fresh:
                x_copy(it, i).wait_send()

    def send_x(it, low, high):
        @pl.when(not_first)
        def _():
            for i, (p, q) in enumerate(pieces[it]):
                if p >= low and q <= high:
                    x_copy(it, i).start()

    def e_copy(it, j):
        low, high = span(plan[it][1], j)
        return remote(
            piece(T.at[it], low, high, TOP), piece(EN.at[it], low, high, 0),
            e_send.at[it, j], e_recv.at[it, j], succ,
        )

    def fin_copy(j):
        low, high = span(plan[-1][3], j)
        return remote(piece(X, low, high, 0), piece(FIN, low, high, 0), fin_send.at[j], fin_recv.at[j], swap)

    def halo_copy(h, side):
        return remote(
            edge_out.at[h, side], edge_in.at[h, side], halo_send.at[h, side], halo_recv.at[h, side],
            bottom_peer if side else top_peer,
        )

    def send_halo(h, side, get):
        def pack():
            for comp in range(3):
                for i in range(HALO):
                    value = get(comp, rows - 1 - i if side else i)
                    edge_out[h, side, comp, i if side else HALO - 1 - i] = -value if comp == 1 else value
            halo_copy(h, side).start()

        if side:
            pack()
        else:
            pl.when(has_top)(pack)

    def take_halo(h, side, buf):
        def unpack():
            halo_copy(h, side).wait()
            at = TOP + rows if side else TOP - HALO
            for comp in range(3):
                buf[comp, at : at + HALO] = edge_in[h, side, comp]

        if side:
            unpack()
        else:
            pl.when(has_top)(unpack)

    send_x(0, 0, rows)
    for side in range(2):
        send_halo(0, side, lambda comp, r: X[comp, r])

    @pl.when(own)
    def _():
        push_e.start()

    def store_d(comp, r, value):
        D[TOP + r] = HALF * value

    @pl.when(own)
    def _():
        each_row(d_own, 1, store_d)

    @pl.when(jnp.logical_not(own))
    def _():
        push_d.wait_recv()
        each_row(stg_d, 1, store_d)


    def edge_line(i, mirrored, line=0):
        plain, back = i // 8 * 64 + i % 8, (15 - i) // 8 * 64 + (15 - i) % 8
        return pl.ds(line + jnp.where(mirrored, back, plain), 8, stride=8)

    def take_bottom(ref, line):
        for i in range(HALO):
            D[TOP + rows + i] = HALF * ref[edge_line(i, flip, line), :]

    @pl.when(own)
    def _():
        push_bottom.wait_recv()
        take_bottom(d_bottom, 0)

    @pl.when(jnp.logical_not(own))
    def _():
        take_bottom(d_own, jnp.where(flip, rows * 8 - 128, 0))

    @pl.when(has_top)
    def _():
        push_top[0].wait_recv()
        for i in range(HALO):
            D[TOP - 1 - i] = HALF * d_top[edge_line(i, jnp.logical_not(flip)), :]

    def run_forward(it, j):
        ends = plan[it][0]
        n = len(ends)
        if j == 0:
            take_halo(2 * it, 0, T.at[it])
        if j == n - 1:
            take_halo(2 * it, 1, T.at[it])
        low = TOP + ends[j - 1] if j else TOP - HALO + 2
        forward(T.at[it], D, F, low, TOP + ends[j], None if j else edge)
        pl.when(not_last)(lambda: e_copy(it, j).start())

    def send_edge(it, side):
        if side:
            need_x(it, rows - HALO, rows)
        else:
            early = some(arrived, it, 0, HALO)
            pl.when(not_last & has_top)(lambda: [x_copy(it, i).wait_recv() for i in early] and None)
            late[it] = early

        def get(comp, r):
            value = E[comp, r] * (XN[it, comp, r] - T[it, comp, TOP + r])
            return jnp.where(not_last, value, 0.0)

        send_halo(2 * it + 1, side, get)

    def run_adjoint(it, j):
        ends = plan[it][1]
        n = len(ends)
        low, high = span(ends, j)
        need_x(it, low, high)
        if j == 0:
            top_free = jnp.logical_not(has_top)
            pl.when(not_last & top_free)(lambda: [x_copy(it, i).wait_recv() for i in late[it]] and None)

        def differ(r, carry):
            at, wide = pl.ds(r, 4), pl.ds(TOP + r, 4)
            for comp in range(3):
                value = E[comp, at] * (XN[it, comp, at] - T[it, comp, wide])
                A[it, comp, wide] = jnp.where(not_last, value, 0.0)
            return carry

        blocks(low, high, 4, differ)
        if j == 0:
            take_halo(2 * it + 1, 0, A.at[it])
        if j == n - 1:
            take_halo(2 * it + 1, 1, A.at[it])
        low = TOP + low if j else TOP - HALO + 2
        adjoint(A.at[it], D, F, low, TOP + plan[it][2][j], None if j else edge)

    def run_update(it, j, acc):
        ends = plan[it][3]
        n = len(ends)
        final = it == ITERS - 1
        low, high = span(ends, j)

        @pl.when(not_first)
        def _():
            e_copy(it, j).wait_recv()

        need_sent(it, low, high)

        def update(r, acc):
            at, wide = pl.ds(r, 4), pl.ds(TOP + r, 4)
            for comp in range(3):
                x = X[comp, at]
                gap = x - EN[it, comp, at]
                lam = E[comp, at] * gap
                wy = WY[comp, at]
                grad = W[comp, at] * x - wy
                acc = acc + 0.5 * jnp.sum(lam * gap + x * (grad - wy), axis=0)
                x = x - STEP_SIZE * (lam - A[it, comp, wide] + grad)
                X[comp, at] = x
                if not final:
                    T[it + 1, comp, wide] = x
            return acc

        if high > low:
            acc = blocks(low, high, 4, update, acc)
            if final:
                pl.when(jnp.logical_not(own))(lambda: fin_copy(j).start())
            else:
                send_x(it + 1, low, high)
        if not final and j == 0:
            send_halo(2 * it + 2, 0, lambda comp, r: X[comp, r])
        if not final and j == n - 1:
            send_halo(2 * it + 2, 1, lambda comp, r: X[comp, r])
        return acc

    for j in range(len(plan[0][0])):
        run_forward(0, j)

    @pl.when(own)
    def _():
        push_d.wait_send()
        push_e.wait_send()
        pl.when(has_top)(lambda: [push.wait_send() for push in push_top] and None)

    @pl.when(jnp.logical_not(own))
    def _():
        push_e.wait_recv()
        push_bottom.wait_send()

    def store_e(comp, r, value):
        E[comp, r] = value

    pl.when(own)(lambda: each_row(e_own, 3, store_e))
    pl.when(jnp.logical_not(own))(lambda: each_row(stg_e, 3, store_e))

    pl.when(push_start)(lambda: push_s.wait_send())
    pl.when(need_start)(lambda: push_s.wait_recv())

    def store_s(comp, r, value):
        if comp == 1:
            value = value * sign
        EN[0, comp, r] = value
        EN[1, comp, r] = value

    pl.when(own_start)(lambda: each_row(s_own, 3, store_s))
    pl.when(need_start)(lambda: each_row(stg_s, 3, store_s))

    acc = [0.5 * c0_ref[...] for _ in range(ITERS)]
    send_edge(0, 0)
    send_edge(0, 1)
    for token in SCHEDULE:
        kind, it, j = token[0], int(token[1]), int(token[2])
        if kind == "F":
            run_forward(it, j)
        elif kind == "E":
            send_edge(it, j)
        elif kind == "A":
            run_adjoint(it, j)
        else:
            acc[it] = run_update(it, j, acc[it])
    for it in range(ITERS):
        cbuf[it] = acc[it]

    def c_copy(s):
        return remote(cbuf, crecv.at[band], c_send.at[s], c_recv.at[band], (2 * y + c, s))

    for s in range(bands):

        @pl.when(jnp.logical_not(own & (sp == s)))
        def _(s=s):
            c_copy(s).start()

    @pl.when(own)
    def _():
        crecv[band] = cbuf[...]

    flip_out = c == 1

    sign_out = jnp.where(flip_out, -1.0, 1.0).astype(jnp.float32)

    def put(src, j):
        low, high = span(plan[-1][3], j)

        def body(r, carry):
            for comp in range(3):
                for i in range(8):
                    value = src[comp, r + i]
                    line = jnp.where(flip_out, (rows - 8 - r) * 8 + 7 - i, r * 8 + i)
                    at = pl.ds(comp * rows * 8 + line, 8, stride=8)
                    OUT[at, :] = value * sign_out if comp == 1 else value
            return carry

        blocks(low, high, 8, body)

    used = [j for j in range(len(plan[-1][3])) if span(plan[-1][3], j)[1] > span(plan[-1][3], j)[0]]
    for j in used:

        @pl.when(own)
        def _():
            put(X, j)

        @pl.when(jnp.logical_not(own))
        def _():
            fin_copy(j).wait_recv()
            put(FIN, j)

    for s in range(bands):

        @pl.when(jnp.logical_not(own & (sp == s)))
        def _(s=s):
            c_copy(s).wait_send()

        @pl.when(jnp.logical_not(own & (band == s)))
        def _(s=s):
            remote(cbuf, crecv.at[s], c_send.at[s], c_recv.at[s], partner).wait_recv()

    total = crecv[0]
    for s in range(1, bands):
        total = total + crecv[s]
    for it in range(ITERS):
        cost_ref[0, it] = jnp.sum(total[it]) / cells

    @pl.when(not_last)
    def _():
        for it in range(ITERS):
            for j in range(len(plan[it][1])):
                e_copy(it, j).wait_send()

    @pl.when(jnp.logical_not(own))
    def _():
        for j in used:
            fin_copy(j).wait_send()


def as_tiles(x):
    x = x.reshape(-1, 8, x.shape[-1] // 128, 128)
    return x.transpose(0, 2, 1, 3).reshape(-1, 128)


def from_tiles(x, shape):
    x = x.reshape(-1, shape[-1] // 128, 8, 128)
    return x.transpose(0, 2, 1, 3).reshape(shape)


def per_device(
    increments, start_state, depth, error_weight, obs_index, obs_count, obs_value, obs_weight
):
    rows, columns = increments.shape[2:]
    slots = obs_index.shape[1]
    bands, windows = lax.axis_size("space"), lax.axis_size("tm")
    pairs = windows // 2
    total_rows = rows * bands
    cells = 3 * total_rows * columns
    _, _, a, y, b, c, band, _ = place()
    own = a == c

    exchange = []
    for py in range(pairs):
        for pb in range(bands // 2):
            one = 2 * py * bands + 2 * pb + 1
            two = (2 * py + 1) * bands + 2 * pb
            exchange += [(one, two), (two, one)]
    both = ("tm", "space")

    live = jnp.arange(slots) < obs_count[0]
    packed = jnp.stack(
        [obs_index[0].astype(jnp.float32), jnp.where(live, obs_weight[0], 0.0), obs_value[0]]
    )
    packed = lax.optimization_barrier(packed)
    packed_got = lax.ppermute(packed, both, exchange)
    x_got = lax.ppermute(increments, both, exchange)
    packed = jnp.where(own, packed, packed_got)

    index = packed[0].astype(jnp.int32)
    component = index // (total_rows * columns)
    line = index // columns % total_rows - band * rows
    inside = (line >= 0) & (line < rows)
    flip = a == 1
    line = jnp.where(flip, rows - 1 - line, line)
    code = (component * rows + jnp.clip(line, 0, rows - 1)) * columns + index % columns
    weight = jnp.where(inside, packed[1], 0.0)
    weighted = weight * packed[2]
    c0 = jnp.sum((weighted * packed[2]).reshape(-1, 8, 128), 0)
    weighted = jnp.where(flip & (component == 1), -weighted, weighted)

    wide = rows + 2 * TOP
    line = jnp.arange(wide) - TOP
    line = band * rows + jnp.where(flip, rows - 1 - line, line)
    latitude = (line.astype(jnp.float32) + 0.5) / total_rows
    rate = CORIOLIS_MAX * jnp.sin(latitude * math.pi - math.pi / 2)
    rate = jnp.where(flip, -rate, rate)
    rate = jnp.broadcast_to(rate[:, None, None], (wide, 8, 128))
    code, weight, weighted, rate, c0 = lax.optimization_barrier((code, weight, weighted, rate, c0))

    lines = 3 * rows * 8
    smem = pl.BlockSpec(memory_space=pltpu.SMEM)
    vmem = pl.BlockSpec(memory_space=pltpu.VMEM)
    grid_type = jax.ShapeDtypeStruct((lines, 128), jnp.float32)
    grid_w, grid_wy = pl.pallas_call(
        functools.partial(deposit_kernel, slots),
        out_shape=(grid_type, grid_type),
        in_specs=[smem] * 3,
        out_specs=(vmem, vmem),
        scratch_shapes=[pltpu.VMEM((lines, 128), jnp.float32)] * (2 * STREAMS - 2),
        compiler_params=pltpu.CompilerParams(vmem_limit_bytes=16 * 2**20),
        cost_estimate=pl.CostEstimate(flops=10**10, bytes_accessed=10**8, transcendentals=0),
        name="deposit",
    )(code, weight, weighted)

    def rows_of(count, lead=(3,)):
        return pltpu.VMEM((*lead, count, 8, 128), jnp.float32)

    tiles = pltpu.VMEM((lines, 128), jnp.float32)
    dma = pltpu.SemaphoreType.DMA
    chunks = len(limits(rows)[-1][0])
    sends = max(map(len, sent_pieces(rows)))
    halo = (HALO, 8, 128)
    out, costs = pl.pallas_call(
        functools.partial(main_kernel, rows, cells, pairs, bands),
        out_shape=(grid_type, jax.ShapeDtypeStruct((1, ITERS), jnp.float32)),
        in_specs=[vmem] * 9,
        out_specs=(vmem, smem),
        scratch_shapes=[
            tiles, pltpu.VMEM((rows * 8, 128), jnp.float32), tiles,
            rows_of(rows), rows_of(wide, (ITERS, 3)), rows_of(wide, (ITERS, 3)),
            rows_of(wide, ()), rows_of(rows),
            rows_of(rows, (ITERS, 3)), rows_of(rows, (ITERS, 3)), rows_of(rows),
            pltpu.VMEM((ITERS, 8, 128), jnp.float32), pltpu.VMEM((bands, ITERS, 8, 128), jnp.float32),
            pltpu.VMEM((2 * ITERS, 2, 3, *halo), jnp.float32), pltpu.VMEM((2 * ITERS, 2, 3, *halo), jnp.float32),
            pltpu.VMEM((128, 128), jnp.float32), pltpu.VMEM((128, 128), jnp.float32),
            dma((6,)), dma((5,)), dma((2 * ITERS, 2)), dma((2 * ITERS, 2)),
            dma((ITERS, sends)), dma((ITERS, sends)), dma((ITERS, chunks)), dma((ITERS, chunks)),
            dma((chunks,)), dma((chunks,)), dma((bands,)), dma((bands,)),
        ],
        compiler_params=pltpu.CompilerParams(
            collective_id=0, has_side_effects=True, vmem_limit_bytes=VMEM * 2**20
        ),
        name="iterations",
    )(
        as_tiles(increments), as_tiles(x_got), as_tiles(error_weight), as_tiles(depth),
        as_tiles(start_state), grid_w.reshape(3, rows, 8, 128), grid_wy.reshape(3, rows, 8, 128),
        rate, c0,
    )
    return from_tiles(out, increments.shape), costs.T


def solution(mesh):
    placed = (
        P("tm", None, "space", None),
        P(None, "space", None),
        P("space", None),
        P(None, "space", None),
        P("tm", None),
        P("tm"),
        P("tm", None),
        P("tm", None),
    )
    return jax.shard_map(
        per_device,
        mesh=mesh,
        in_specs=placed,
        out_specs=(P("tm", None, "space", None), P(None, "tm")),
        check_vma=False,
    )
```

```python
import functools
import math

import jax
import jax.numpy as jnp
from jax import lax
from jax.experimental import pallas as pl
from jax.experimental.pallas import tpu as pltpu
from jax.sharding import PartitionSpec as P

STEPS = 6
ITERS = 2
COURANT = 0.35
HALF = 0.5 * COURANT
CORIOLIS_MAX = 0.2
STEP_SIZE = 0.2
HALO = 2 * STEPS
TOP = 24
BLK = 8
STREAMS = 2
UNROLL = 16
VMEM = 36
SCHEDULE = (
    "E00", "A00", "U00", "E01", "A01", "U01", "A02", "U02", "F10",
    "E10", "F11", "A03", "U03", "F12", "F13", "A10", "U10", "A11",
    "U11", "A12", "U12", "F14", "E11", "A13", "U13", "A14", "U14",
)
MESH = pl.DeviceIdType.MESH


def dlon(f):
    lane = lax.broadcasted_iota(jnp.int32, f.shape, 2)
    g = pltpu.roll(f, 127, axis=2)
    g = jnp.where(lane == 127, pltpu.roll(g, 7, axis=1), g)
    m = pltpu.roll(f, 1, axis=2)
    m = jnp.where(lane == 0, pltpu.roll(m, 1, axis=1), m)
    return g - m


def slab(T, low, high, first, second, edge):
    for s in range(STEPS):
        for r in range(low, high, BLK):
            first(r - 1 - 2 * s, min(BLK, high - r))
        if edge is not None:
            T[2, TOP - 1] = T[2, TOP - 1] * edge
        for r in range(low, high, BLK):
            second(r - 2 - 2 * s, min(BLK, high - r))


def forward(T, D, F, low, high, edge):
    def first(r, n):
        at = pl.ds(r, n)
        above, below = pl.ds(r + 1, n), pl.ds(r - 1, n)
        du = D[at] * T[0, at]
        T[2, at] = T[2, at] - (dlon(du) + (D[above] * T[1, above] - D[below] * T[1, below]))

    def second(r, n):
        at = pl.ds(r, n)
        f = F[at]
        v = T[1, at]
        u = T[0, at] + f * v - HALF * dlon(T[2, at])
        T[0, at] = u
        T[1, at] = v - f * u - HALF * (T[2, pl.ds(r + 1, n)] - T[2, pl.ds(r - 1, n)])

    slab(T, low, high, first, second, edge)


def adjoint(T, D, F, low, high, edge):
    def first(r, n):
        at = pl.ds(r, n)
        a = T[0, at] - F[at] * T[1, at]
        T[0, at] = a
        T[2, at] = T[2, at] + HALF * ((T[1, pl.ds(r + 1, n)] - T[1, pl.ds(r - 1, n)]) + dlon(a))

    def second(r, n):
        at = pl.ds(r, n)
        a = T[0, at]
        d = D[at]
        T[0, at] = a + d * dlon(T[2, at])
        T[1, at] = T[1, at] + F[at] * a + d * (T[2, pl.ds(r + 1, n)] - T[2, pl.ds(r - 1, n)])

    slab(T, low, high, first, second, edge)


def deposit_kernel(count, code_ref, w_ref, wy_ref, out_w, out_wy, *more):
    grids = [(out_w, out_wy)] + [(more[2 * i], more[2 * i + 1]) for i in range(STREAMS - 1)]
    total = out_w.shape[0]
    zero = jnp.zeros((64, 128), jnp.float32)

    def clear(i, carry):
        at = pl.ds(pl.multiple_of(i * 64, 64), 64)
        for gw, gy in grids:
            gw[at, :] = zero
            gy[at, :] = zero
        return carry

    lax.fori_loop(0, total // 64, clear, 0)
    lanes = lax.broadcasted_iota(jnp.int32, (1, 128), 1)

    def add(i, carry):
        for k in range(UNROLL):
            for s, (gw, gy) in enumerate(grids):
                j = (i * UNROLL + k) * STREAMS + s
                code = code_ref[j]
                at = pl.ds(lax.shift_right_logical(code, 7), 1)
                hit = lanes == (code & 127)
                gw[at, :] = gw[at, :] + jnp.where(hit, w_ref[j], 0.0)
                gy[at, :] = gy[at, :] + jnp.where(hit, wy_ref[j], 0.0)
        return carry

    lax.fori_loop(0, count // (STREAMS * UNROLL), add, 0)

    def gather(i, carry):
        at = pl.ds(pl.multiple_of(i * 64, 64), 64)
        out_w[at, :] = sum([g[0][at, :] for g in grids[1:]], out_w[at, :])
        out_wy[at, :] = sum([g[1][at, :] for g in grids[1:]], out_wy[at, :])
        return carry

    lax.fori_loop(0, total // 64, gather, 0)


def place():
    tm, sp = lax.axis_index("tm"), lax.axis_index("space")
    a, y, b, c = tm % 2, tm // 2, sp // 2, sp % 2
    return tm, sp, a, y, b, c, 2 * b + a, 2 * y + c


def limits(rows):
    forward_high = [rows * 3 // 8, rows * 5 // 8, rows * 7 // 8, rows + HALO]
    plan = []
    for _ in range(ITERS):
        e = [r - HALO for r in forward_high]
        adjoint_high = e[:-1] + [rows + HALO]
        u = [r - HALO for r in adjoint_high]
        plan.append((forward_high, e, adjoint_high, u))
        forward_high = u + [rows + HALO]
    return plan


def early_rows(rows):
    return limits(rows)[0][0][1]


def sent_pieces(rows):
    edge = rows - HALO
    plan = limits(rows)
    x, later = plan[0][0], plan[0][3]
    first = [(0, HALO), (edge, rows), (HALO, x[0])] + list(zip(x[:-2], x[1:-1])) + [(x[-2], edge)]
    then = list(zip([0] + later[:-2], later[:-1])) + [(edge, rows), (later[-2], edge)]
    return first, then


def main_kernel(
    rows, cells, pairs, bands,
    x_own, x_got, e_own, d_own, s_own, W, WY, F, c0_ref,
    OUT, cost_ref,
    stg_r, stg_e, stg_d, stg_s, X, T, A, D, E, XN, EN, FIN, cbuf, crecv,
    edge_out, edge_in, d_top, d_bottom,
    push_send, push_recv, rest_send, rest_recv, halo_send, halo_recv,
    x_send, x_recv, e_send, e_recv, fin_send, fin_recv, c_send, c_recv,
):
    tm, sp, a, y, b, c, band, window = place()
    last = 2 * pairs - 1
    own = a == c
    partner = (tm, 2 * b + (1 - c))
    swap = (2 * y + (1 - a), 2 * b + (1 - c))
    flip = a == 1
    sign = jnp.where(flip, -1.0, 1.0).astype(jnp.float32)
    bottom_peer = (2 * y + (1 - a), sp)
    top_band = jnp.where(flip, band + 1, band - 1)
    has_top = (top_band >= 0) & (top_band < bands)
    top_band = lax.rem(top_band + bands, bands)
    top_peer = (2 * y + top_band % 2, 2 * (top_band // 2) + c)
    succ_y = lax.rem(y + c, pairs)
    succ = (2 * succ_y + a, 2 * b + (1 - c))
    pred_y = lax.rem(y + pairs - (1 - c), pairs)
    pred = (2 * pred_y + a, 2 * b + (1 - c))
    not_first, not_last = window > 0, window < last
    edge = jnp.where(has_top, 1.0, 0.0).astype(jnp.float32)
    plan = limits(rows)
    pieces = sent_pieces(rows)
    part = early_rows(rows)
    rest = rows - part

    edge_lines = pl.ds(pl.multiple_of(jnp.where(flip, rows * 8 - 128, 0), 128), 128)
    own_start = own & (y == 0) & (c == 0)
    push_start = own & (y == 0) & (c == 1)
    need_start = jnp.logical_not(own) & (y == 0) & (c == 0)

    barrier = pltpu.get_barrier_semaphore()
    for da in range(2):
        for s in range(bands):
            other = jnp.logical_not((a == da) & (sp == s))

            @pl.when(other)
            def _(da=da, s=s):
                pl.semaphore_signal(barrier, inc=1, device_id=(2 * y + da, s), device_id_type=MESH)

    far = jnp.where(c == 1, not_last, not_first)
    far_y = jnp.where(c == 1, succ_y, pred_y)

    @pl.when(far)
    def _():
        pl.semaphore_signal(
            barrier, inc=1, device_id=(2 * far_y + a, 2 * b + (1 - c)), device_id_type=MESH
        )

    zeros = jnp.zeros((TOP, 8, 128), jnp.float32)
    D[0:TOP] = zeros
    for it in range(ITERS):
        for i in range(3):
            T[it, i, 0:TOP] = zeros
            A[it, i, 0:TOP] = zeros

    def blocks(low, high, size, body, init=0):
        return lax.fori_loop(
            0, (high - low) // size, lambda i, carry: body(low + i * size, carry), init
        )

    def each_row(stage, comps, count, store, first=0):
        def body(r, carry):
            for comp in range(comps):
                for j in range(8):
                    line = jnp.where(flip, (count - 8 - r) * 8 + 7 - j, r * 8 + j)
                    value = stage[pl.ds(comp * count * 8 + line, 8, stride=8), :]
                    store(comp, first + r + j, value)
            return carry

        blocks(0, count, 8, body)

    def store_x(comp, r, value):
        if comp == 1:
            value = value * sign
        X[comp, r] = value
        T[0, comp, TOP + r] = value

    @pl.when(own)
    def _():
        each_row(x_own, 3, rows, store_x)

    @pl.when(jnp.logical_not(own))
    def _():
        each_row(x_got, 3, part, store_x)

    pl.semaphore_wait(barrier, 2 * bands - 1 + far.astype(jnp.int32))

    def remote(src, dst, send, recv, to):
        return pltpu.make_async_remote_copy(
            src_ref=src, dst_ref=dst, send_sem=send, recv_sem=recv, device_id=to, device_id_type=MESH
        )

    rest_line = pl.multiple_of(jnp.where(flip, part * 8, 0), 128)
    rests = [
        remote(
            x_own.at[pl.ds(comp * rows * 8 + rest_line, rest * 8)],
            stg_r.at[pl.ds(comp * rest * 8, rest * 8)],
            rest_send.at[comp], rest_recv.at[comp], swap,
        )
        for comp in range(3)
    ]

    @pl.when(jnp.logical_not(own))
    def _():
        for copy in rests:
            copy.start()

    push_e = remote(e_own, stg_e, push_send.at[0], push_recv.at[0], partner)
    push_d = remote(d_own, stg_d, push_send.at[1], push_recv.at[1], partner)
    push_s = remote(s_own, stg_s, push_send.at[2], push_recv.at[2], partner)

    push_bottom = remote(d_own.at[edge_lines], d_bottom, push_send.at[3], push_recv.at[3], partner)
    push_top = [
        remote(
            d_own.at[edge_lines], d_top, push_send.at[4 + i], push_recv.at[4], (top_peer[0], 2 * (top_band // 2) + i)
        )
        for i in range(2)
    ]

    @pl.when(own)
    def _():
        push_d.start()
        pl.when(has_top)(lambda: [push.start() for push in push_top] and None)

    @pl.when(jnp.logical_not(own))
    def _():
        push_bottom.start()

    @pl.when(push_start)
    def _():
        push_s.start()

    def piece(ref, low, high, top):
        return ref.at[:, pl.ds(top + low, high - low)]

    def span(ends, j):
        return (ends[j - 1] if j else 0), ends[j]

    def x_copy(it, i):
        low, high = pieces[it][i]
        return remote(
            piece(X, low, high, 0), piece(XN.at[it], low, high, 0), x_send.at[it, i], x_recv.at[it, i], pred
        )

    arrived, sent, late = set(), set(), {}

    def some(done, it, low, high):
        fresh = [i for i, (p, q) in enumerate(pieces[it]) if p < high and q > low and (it, i) not in done]
        done.update((it, i) for i in fresh)
        return fresh

    def need_x(it, low, high):
        fresh = some(arrived, it, low, high)

        @pl.when(not_last)
        def _():
            for i in fresh:
                x_copy(it, i).wait_recv()

    def need_sent(it, low, high):
        fresh = some(sent, it, low, high)

        @pl.when(not_first)
        def _():
            for i in fresh:
                x_copy(it, i).wait_send()

    def send_x(it, low, high, late=None):
        @pl.when(not_first)
        def _():
            for i, (p, q) in enumerate(pieces[it]):
                if p >= low and q <= high and (late is None or late == (q > part)):
                    x_copy(it, i).start()

    def e_copy(it, j):
        low, high = span(plan[it][1], j)
        return remote(
            piece(T.at[it], low, high, TOP), piece(EN.at[it], low, high, 0),
            e_send.at[it, j], e_recv.at[it, j], succ,
        )

    def fin_copy(j):
        low, high = span(plan[-1][3], j)
        return remote(piece(X, low, high, 0), piece(FIN, low, high, 0), fin_send.at[j], fin_recv.at[j], swap)

    def halo_copy(h, side):
        return remote(
            edge_out.at[h, side], edge_in.at[h, side], halo_send.at[h, side], halo_recv.at[h, side],
            bottom_peer if side else top_peer,
        )

    def send_halo(h, side, get):
        def pack():
            for comp in range(3):
                for i in range(HALO):
                    value = get(comp, rows - 1 - i if side else i)
                    edge_out[h, side, comp, i if side else HALO - 1 - i] = -value if comp == 1 else value
            halo_copy(h, side).start()

        if side:
            pack()
        else:
            pl.when(has_top)(pack)

    def take_halo(h, side, buf):
        def unpack():
            halo_copy(h, side).wait()
            at = TOP + rows if side else TOP - HALO
            for comp in range(3):
                buf[comp, at : at + HALO] = edge_in[h, side, comp]

        if side:
            unpack()
        else:
            pl.when(has_top)(unpack)

    send_x(0, 0, part, False)
    send_halo(0, 0, lambda comp, r: X[comp, r])

    def send_late():
        send_x(0, 0, rows, True)
        send_halo(0, 1, lambda comp, r: X[comp, r])

    pl.when(own)(send_late)

    @pl.when(own)
    def _():
        push_e.start()

    def store_d(comp, r, value):
        D[TOP + r] = HALF * value

    @pl.when(own)
    def _():
        each_row(d_own, 1, rows, store_d)

    @pl.when(jnp.logical_not(own))
    def _():
        push_d.wait_recv()
        each_row(stg_d, 1, rows, store_d)


    def edge_line(i, mirrored, line=0):
        plain, back = i // 8 * 64 + i % 8, (15 - i) // 8 * 64 + (15 - i) % 8
        return pl.ds(line + jnp.where(mirrored, back, plain), 8, stride=8)

    def take_bottom(ref, line):
        for i in range(HALO):
            D[TOP + rows + i] = HALF * ref[edge_line(i, flip, line), :]

    @pl.when(own)
    def _():
        push_bottom.wait_recv()
        take_bottom(d_bottom, 0)

    @pl.when(jnp.logical_not(own))
    def _():
        take_bottom(d_own, jnp.where(flip, rows * 8 - 128, 0))

    @pl.when(has_top)
    def _():
        push_top[0].wait_recv()
        for i in range(HALO):
            D[TOP - 1 - i] = HALF * d_top[edge_line(i, jnp.logical_not(flip)), :]

    def run_forward(it, j):
        ends = plan[it][0]
        n = len(ends)
        if j == 0:
            take_halo(2 * it, 0, T.at[it])
        if j == n - 1:
            take_halo(2 * it, 1, T.at[it])
        low = TOP + ends[j - 1] if j else TOP - HALO + 2
        forward(T.at[it], D, F, low, TOP + ends[j], None if j else edge)
        pl.when(not_last)(lambda: e_copy(it, j).start())

    def send_edge(it, side):
        if side:
            need_x(it, rows - HALO, rows)
        else:
            early = some(arrived, it, 0, HALO)
            pl.when(not_last & has_top)(lambda: [x_copy(it, i).wait_recv() for i in early] and None)
            late[it] = early

        def get(comp, r):
            value = E[comp, r] * (XN[it, comp, r] - T[it, comp, TOP + r])
            return jnp.where(not_last, value, 0.0)

        send_halo(2 * it + 1, side, get)

    def run_adjoint(it, j):
        ends = plan[it][1]
        n = len(ends)
        low, high = span(ends, j)
        need_x(it, low, high)
        if j == 0:
            top_free = jnp.logical_not(has_top)
            pl.when(not_last & top_free)(lambda: [x_copy(it, i).wait_recv() for i in late[it]] and None)

        def differ(r, carry):
            at, wide = pl.ds(r, 4), pl.ds(TOP + r, 4)
            for comp in range(3):
                value = E[comp, at] * (XN[it, comp, at] - T[it, comp, wide])
                A[it, comp, wide] = jnp.where(not_last, value, 0.0)
            return carry

        blocks(low, high, 4, differ)
        if j == 0:
            take_halo(2 * it + 1, 0, A.at[it])
        if j == n - 1:
            take_halo(2 * it + 1, 1, A.at[it])
        low = TOP + low if j else TOP - HALO + 2
        adjoint(A.at[it], D, F, low, TOP + plan[it][2][j], None if j else edge)

    def run_update(it, j, acc):
        ends = plan[it][3]
        n = len(ends)
        final = it == ITERS - 1
        low, high = span(ends, j)

        @pl.when(not_first)
        def _():
            e_copy(it, j).wait_recv()

        need_sent(it, low, high)

        def update(r, acc):
            at, wide = pl.ds(r, 4), pl.ds(TOP + r, 4)
            for comp in range(3):
                x = X[comp, at]
                gap = x - EN[it, comp, at]
                lam = E[comp, at] * gap
                wy = WY[comp, at]
                grad = W[comp, at] * x - wy
                acc = acc + 0.5 * jnp.sum(lam * gap + x * (grad - wy), axis=0)
                x = x - STEP_SIZE * (lam - A[it, comp, wide] + grad)
                X[comp, at] = x
                if not final:
                    T[it + 1, comp, wide] = x
            return acc

        if high > low:
            acc = blocks(low, high, 4, update, acc)
            if final:
                pl.when(jnp.logical_not(own))(lambda: fin_copy(j).start())
            else:
                send_x(it + 1, low, high)
        if not final and j == 0:
            send_halo(2 * it + 2, 0, lambda comp, r: X[comp, r])
        if not final and j == n - 1:
            send_halo(2 * it + 2, 1, lambda comp, r: X[comp, r])
        return acc

    def take_rest():
        for copy in rests:
            copy.wait()
        each_row(stg_r, 3, rest, store_x, part)
        send_late()

    for j, high in enumerate(plan[0][0]):
        if j and plan[0][0][j - 1] == part:
            pl.when(jnp.logical_not(own))(take_rest)
        run_forward(0, j)

    @pl.when(own)
    def _():
        push_d.wait_send()
        push_e.wait_send()
        pl.when(has_top)(lambda: [push.wait_send() for push in push_top] and None)

    @pl.when(jnp.logical_not(own))
    def _():
        push_e.wait_recv()
        push_bottom.wait_send()

    def store_e(comp, r, value):
        E[comp, r] = value

    pl.when(own)(lambda: each_row(e_own, 3, rows, store_e))
    pl.when(jnp.logical_not(own))(lambda: each_row(stg_e, 3, rows, store_e))

    pl.when(push_start)(lambda: push_s.wait_send())
    pl.when(need_start)(lambda: push_s.wait_recv())

    def store_s(comp, r, value):
        if comp == 1:
            value = value * sign
        EN[0, comp, r] = value
        EN[1, comp, r] = value

    pl.when(own_start)(lambda: each_row(s_own, 3, rows, store_s))
    pl.when(need_start)(lambda: each_row(stg_s, 3, rows, store_s))

    acc = [0.5 * c0_ref[...] for _ in range(ITERS)]
    for token in SCHEDULE:
        kind, it, j = token[0], int(token[1]), int(token[2])
        if kind == "F":
            run_forward(it, j)
        elif kind == "E":
            send_edge(it, j)
        elif kind == "A":
            run_adjoint(it, j)
        else:
            acc[it] = run_update(it, j, acc[it])
    for it in range(ITERS):
        cbuf[it] = acc[it]

    def c_copy(s):
        return remote(cbuf, crecv.at[band], c_send.at[s], c_recv.at[band], (2 * y + c, s))

    for s in range(bands):

        @pl.when(jnp.logical_not(own & (sp == s)))
        def _(s=s):
            c_copy(s).start()

    @pl.when(own)
    def _():
        crecv[band] = cbuf[...]

    flip_out = c == 1

    sign_out = jnp.where(flip_out, -1.0, 1.0).astype(jnp.float32)

    def put(src, j):
        low, high = span(plan[-1][3], j)

        def body(r, carry):
            for comp in range(3):
                for i in range(8):
                    value = src[comp, r + i]
                    line = jnp.where(flip_out, (rows - 8 - r) * 8 + 7 - i, r * 8 + i)
                    at = pl.ds(comp * rows * 8 + line, 8, stride=8)
                    OUT[at, :] = value * sign_out if comp == 1 else value
            return carry

        blocks(low, high, 8, body)

    used = [j for j in range(len(plan[-1][3])) if span(plan[-1][3], j)[1] > span(plan[-1][3], j)[0]]
    for j in used:

        @pl.when(own)
        def _():
            put(X, j)

        @pl.when(jnp.logical_not(own))
        def _():
            fin_copy(j).wait_recv()
            put(FIN, j)

    for s in range(bands):

        @pl.when(jnp.logical_not(own & (sp == s)))
        def _(s=s):
            c_copy(s).wait_send()

        @pl.when(jnp.logical_not(own & (band == s)))
        def _(s=s):
            remote(cbuf, crecv.at[s], c_send.at[s], c_recv.at[s], partner).wait_recv()

    total = crecv[0]
    for s in range(1, bands):
        total = total + crecv[s]
    for it in range(ITERS):
        cost_ref[0, it] = jnp.sum(total[it]) / cells

    @pl.when(not_last)
    def _():
        for it in range(ITERS):
            for j in range(len(plan[it][1])):
                e_copy(it, j).wait_send()

    @pl.when(jnp.logical_not(own))
    def _():
        for j in used:
            fin_copy(j).wait_send()


def as_tiles(x):
    x = x.reshape(-1, 8, x.shape[-1] // 128, 128)
    return x.transpose(0, 2, 1, 3).reshape(-1, 128)


def from_tiles(x, shape):
    x = x.reshape(-1, shape[-1] // 128, 8, 128)
    return x.transpose(0, 2, 1, 3).reshape(shape)


def per_device(
    increments, start_state, depth, error_weight, obs_index, obs_count, obs_value, obs_weight
):
    rows, columns = increments.shape[2:]
    slots = obs_index.shape[1]
    bands, windows = lax.axis_size("space"), lax.axis_size("tm")
    pairs = windows // 2
    total_rows = rows * bands
    cells = 3 * total_rows * columns
    _, _, a, y, b, c, band, _ = place()
    own = a == c

    exchange = []
    for py in range(pairs):
        for pb in range(bands // 2):
            one = 2 * py * bands + 2 * pb + 1
            two = (2 * py + 1) * bands + 2 * pb
            exchange += [(one, two), (two, one)]
    both = ("tm", "space")

    live = jnp.arange(slots) < obs_count[0]
    packed = jnp.stack(
        [obs_index[0].astype(jnp.float32), jnp.where(live, obs_weight[0], 0.0), obs_value[0]]
    )
    packed = lax.optimization_barrier(packed)
    packed_got = lax.ppermute(packed, both, exchange)
    early = early_rows(rows)
    x_early = jnp.where(a == 1, increments[:, :, :early], increments[:, :, rows - early :])
    x_got = lax.ppermute(x_early, both, exchange)
    packed = jnp.where(own, packed, packed_got)

    index = packed[0].astype(jnp.int32)
    component = index // (total_rows * columns)
    line = index // columns % total_rows - band * rows
    inside = (line >= 0) & (line < rows)
    flip = a == 1
    line = jnp.where(flip, rows - 1 - line, line)
    code = (component * rows + jnp.clip(line, 0, rows - 1)) * columns + index % columns
    weight = jnp.where(inside, packed[1], 0.0)
    weighted = weight * packed[2]
    c0 = jnp.sum((weighted * packed[2]).reshape(-1, 8, 128), 0)
    weighted = jnp.where(flip & (component == 1), -weighted, weighted)

    wide = rows + 2 * TOP
    line = jnp.arange(wide) - TOP
    line = band * rows + jnp.where(flip, rows - 1 - line, line)
    latitude = (line.astype(jnp.float32) + 0.5) / total_rows
    rate = CORIOLIS_MAX * jnp.sin(latitude * math.pi - math.pi / 2)
    rate = jnp.where(flip, -rate, rate)
    rate = jnp.broadcast_to(rate[:, None, None], (wide, 8, 128))
    code, weight, weighted, rate, c0 = lax.optimization_barrier((code, weight, weighted, rate, c0))

    lines = 3 * rows * 8
    smem = pl.BlockSpec(memory_space=pltpu.SMEM)
    vmem = pl.BlockSpec(memory_space=pltpu.VMEM)
    grid_type = jax.ShapeDtypeStruct((lines, 128), jnp.float32)
    grid_w, grid_wy = pl.pallas_call(
        functools.partial(deposit_kernel, slots),
        out_shape=(grid_type, grid_type),
        in_specs=[smem] * 3,
        out_specs=(vmem, vmem),
        scratch_shapes=[pltpu.VMEM((lines, 128), jnp.float32)] * (2 * STREAMS - 2),
        compiler_params=pltpu.CompilerParams(vmem_limit_bytes=16 * 2**20),
        cost_estimate=pl.CostEstimate(flops=10**10, bytes_accessed=10**8, transcendentals=0),
        name="deposit",
    )(code, weight, weighted)

    def rows_of(count, lead=(3,)):
        return pltpu.VMEM((*lead, count, 8, 128), jnp.float32)

    tiles = pltpu.VMEM((lines, 128), jnp.float32)
    dma = pltpu.SemaphoreType.DMA
    chunks = len(limits(rows)[-1][0])
    sends = max(map(len, sent_pieces(rows)))
    halo = (HALO, 8, 128)
    out, costs = pl.pallas_call(
        functools.partial(main_kernel, rows, cells, pairs, bands),
        out_shape=(grid_type, jax.ShapeDtypeStruct((1, ITERS), jnp.float32)),
        in_specs=[vmem] * 9,
        out_specs=(vmem, smem),
        scratch_shapes=[
            pltpu.VMEM((3 * (rows - early) * 8, 128), jnp.float32),
            tiles, pltpu.VMEM((rows * 8, 128), jnp.float32), tiles,
            rows_of(rows), rows_of(wide, (ITERS, 3)), rows_of(wide, (ITERS, 3)),
            rows_of(wide, ()), rows_of(rows),
            rows_of(rows, (ITERS, 3)), rows_of(rows, (ITERS, 3)), rows_of(rows),
            pltpu.VMEM((ITERS, 8, 128), jnp.float32), pltpu.VMEM((bands, ITERS, 8, 128), jnp.float32),
            pltpu.VMEM((2 * ITERS, 2, 3, *halo), jnp.float32), pltpu.VMEM((2 * ITERS, 2, 3, *halo), jnp.float32),
            pltpu.VMEM((128, 128), jnp.float32), pltpu.VMEM((128, 128), jnp.float32),
            dma((6,)), dma((5,)), dma((3,)), dma((3,)), dma((2 * ITERS, 2)), dma((2 * ITERS, 2)),
            dma((ITERS, sends)), dma((ITERS, sends)), dma((ITERS, chunks)), dma((ITERS, chunks)),
            dma((chunks,)), dma((chunks,)), dma((bands,)), dma((bands,)),
        ],
        compiler_params=pltpu.CompilerParams(
            collective_id=0, has_side_effects=True, vmem_limit_bytes=VMEM * 2**20
        ),
        name="iterations",
    )(
        as_tiles(increments), as_tiles(x_got), as_tiles(error_weight), as_tiles(depth),
        as_tiles(start_state), grid_w.reshape(3, rows, 8, 128), grid_wy.reshape(3, rows, 8, 128),
        rate, c0,
    )
    return from_tiles(out, increments.shape), costs.T


def solution(mesh):
    placed = (
        P("tm", None, "space", None),
        P(None, "space", None),
        P("space", None),
        P(None, "space", None),
        P("tm", None),
        P("tm"),
        P("tm", None),
        P("tm", None),
    )
    return jax.shard_map(
        per_device,
        mesh=mesh,
        in_specs=placed,
        out_specs=(P("tm", None, "space", None), P(None, "tm")),
        check_vma=False,
    )
```

```python
import functools
import math

import jax
import jax.numpy as jnp
from jax import lax
from jax.experimental import pallas as pl
from jax.experimental.pallas import tpu as pltpu
from jax.sharding import PartitionSpec as P

STEPS = 6
ITERS = 2
COURANT = 0.35
HALF = 0.5 * COURANT
CORIOLIS_MAX = 0.2
STEP_SIZE = 0.2
HALO = 2 * STEPS
TOP = 24
BLK = 8
STREAMS = 2
UNROLL = 16
VMEM = 36
SCHEDULE = (
    "A00", "U00", "A01", "U01", "A02", "U02", "F10",
    "E10", "F11", "A03", "U03", "F12", "F13", "A10", "U10", "A11",
    "U11", "A12", "U12", "F14", "E11", "A13", "U13", "A14", "U14",
)
MESH = pl.DeviceIdType.MESH


def dlon(f):
    lane = lax.broadcasted_iota(jnp.int32, f.shape, 2)
    g = pltpu.roll(f, 127, axis=2)
    g = jnp.where(lane == 127, pltpu.roll(g, 7, axis=1), g)
    m = pltpu.roll(f, 1, axis=2)
    m = jnp.where(lane == 0, pltpu.roll(m, 1, axis=1), m)
    return g - m


def slab(T, low, high, first, second, edge):
    for s in range(STEPS):
        for r in range(low, high, BLK):
            first(r - 1 - 2 * s, min(BLK, high - r))
        if edge is not None:
            T[2, TOP - 1] = T[2, TOP - 1] * edge
        for r in range(low, high, BLK):
            second(r - 2 - 2 * s, min(BLK, high - r))


def forward(T, D, F, low, high, edge):
    def first(r, n):
        at = pl.ds(r, n)
        above, below = pl.ds(r + 1, n), pl.ds(r - 1, n)
        du = D[at] * T[0, at]
        T[2, at] = T[2, at] - (dlon(du) + (D[above] * T[1, above] - D[below] * T[1, below]))

    def second(r, n):
        at = pl.ds(r, n)
        f = F[at]
        v = T[1, at]
        u = T[0, at] + f * v - HALF * dlon(T[2, at])
        T[0, at] = u
        T[1, at] = v - f * u - HALF * (T[2, pl.ds(r + 1, n)] - T[2, pl.ds(r - 1, n)])

    slab(T, low, high, first, second, edge)


def adjoint(T, D, F, low, high, edge):
    def first(r, n):
        at = pl.ds(r, n)
        a = T[0, at] - F[at] * T[1, at]
        T[0, at] = a
        T[2, at] = T[2, at] + HALF * ((T[1, pl.ds(r + 1, n)] - T[1, pl.ds(r - 1, n)]) + dlon(a))

    def second(r, n):
        at = pl.ds(r, n)
        a = T[0, at]
        d = D[at]
        T[0, at] = a + d * dlon(T[2, at])
        T[1, at] = T[1, at] + F[at] * a + d * (T[2, pl.ds(r + 1, n)] - T[2, pl.ds(r - 1, n)])

    slab(T, low, high, first, second, edge)


def deposit_kernel(count, code_ref, w_ref, wy_ref, out_w, out_wy, *more):
    grids = [(out_w, out_wy)] + [(more[2 * i], more[2 * i + 1]) for i in range(STREAMS - 1)]
    total = out_w.shape[0]
    zero = jnp.zeros((64, 128), jnp.float32)

    def clear(i, carry):
        at = pl.ds(pl.multiple_of(i * 64, 64), 64)
        for gw, gy in grids:
            gw[at, :] = zero
            gy[at, :] = zero
        return carry

    lax.fori_loop(0, total // 64, clear, 0)
    lanes = lax.broadcasted_iota(jnp.int32, (1, 128), 1)

    def add(i, carry):
        for k in range(UNROLL):
            for s, (gw, gy) in enumerate(grids):
                j = (i * UNROLL + k) * STREAMS + s
                code = code_ref[j]
                at = pl.ds(lax.shift_right_logical(code, 7), 1)
                hit = lanes == (code & 127)
                gw[at, :] = gw[at, :] + jnp.where(hit, w_ref[j], 0.0)
                gy[at, :] = gy[at, :] + jnp.where(hit, wy_ref[j], 0.0)
        return carry

    lax.fori_loop(0, count // (STREAMS * UNROLL), add, 0)

    def gather(i, carry):
        at = pl.ds(pl.multiple_of(i * 64, 64), 64)
        out_w[at, :] = sum([g[0][at, :] for g in grids[1:]], out_w[at, :])
        out_wy[at, :] = sum([g[1][at, :] for g in grids[1:]], out_wy[at, :])
        return carry

    lax.fori_loop(0, total // 64, gather, 0)


def place():
    tm, sp = lax.axis_index("tm"), lax.axis_index("space")
    a, y, b, c = tm % 2, tm // 2, sp // 2, sp % 2
    return tm, sp, a, y, b, c, 2 * b + a, 2 * y + c


def limits(rows):
    forward_high = [rows * 3 // 8, rows * 5 // 8, rows * 7 // 8, rows + HALO]
    plan = []
    for _ in range(ITERS):
        e = [r - HALO for r in forward_high]
        adjoint_high = e[:-1] + [rows + HALO]
        u = [r - HALO for r in adjoint_high]
        plan.append((forward_high, e, adjoint_high, u))
        forward_high = u + [rows + HALO]
    return plan


def early_rows(rows):
    return limits(rows)[0][0][1]


def sent_pieces(rows):
    edge = rows - HALO
    plan = limits(rows)
    x, later = plan[0][0], plan[0][3]
    first = [(0, HALO), (edge, rows), (HALO, x[0])] + list(zip(x[:-2], x[1:-1])) + [(x[-2], edge)]
    then = list(zip([0] + later[:-2], later[:-1])) + [(edge, rows), (later[-2], edge)]
    return first, then


def main_kernel(
    rows, cells, pairs, bands,
    x_own, x_got, e_own, d_own, s_own, W, WY, F, c0_ref,
    OUT, cost_ref,
    stg_r, stg_e, stg_d, stg_s, X, T, A, D, E, XN, EN, FIN, cbuf, crecv,
    edge_out, edge_in, d_top, d_bottom,
    push_send, push_recv, rest_send, rest_recv, halo_send, halo_recv,
    x_send, x_recv, e_send, e_recv, fin_send, fin_recv, c_send, c_recv,
):
    tm, sp, a, y, b, c, band, window = place()
    last = 2 * pairs - 1
    own = a == c
    partner = (tm, 2 * b + (1 - c))
    swap = (2 * y + (1 - a), 2 * b + (1 - c))
    flip = a == 1
    sign = jnp.where(flip, -1.0, 1.0).astype(jnp.float32)
    bottom_peer = (2 * y + (1 - a), sp)
    top_band = jnp.where(flip, band + 1, band - 1)
    has_top = (top_band >= 0) & (top_band < bands)
    top_band = lax.rem(top_band + bands, bands)
    top_peer = (2 * y + top_band % 2, 2 * (top_band // 2) + c)
    succ_y = lax.rem(y + c, pairs)
    succ = (2 * succ_y + a, 2 * b + (1 - c))
    pred_y = lax.rem(y + pairs - (1 - c), pairs)
    pred = (2 * pred_y + a, 2 * b + (1 - c))
    not_first, not_last = window > 0, window < last
    edge = jnp.where(has_top, 1.0, 0.0).astype(jnp.float32)
    plan = limits(rows)
    pieces = sent_pieces(rows)
    part = early_rows(rows)
    rest = rows - part

    edge_lines = pl.ds(pl.multiple_of(jnp.where(flip, rows * 8 - 128, 0), 128), 128)
    own_start = own & (y == 0) & (c == 0)
    push_start = own & (y == 0) & (c == 1)
    need_start = jnp.logical_not(own) & (y == 0) & (c == 0)

    barrier = pltpu.get_barrier_semaphore()
    for da in range(2):
        for s in range(bands):
            other = jnp.logical_not((a == da) & (sp == s))

            @pl.when(other)
            def _(da=da, s=s):
                pl.semaphore_signal(barrier, inc=1, device_id=(2 * y + da, s), device_id_type=MESH)

    far = jnp.where(c == 1, not_last, not_first)
    far_y = jnp.where(c == 1, succ_y, pred_y)

    @pl.when(far)
    def _():
        pl.semaphore_signal(
            barrier, inc=1, device_id=(2 * far_y + a, 2 * b + (1 - c)), device_id_type=MESH
        )

    zeros = jnp.zeros((TOP, 8, 128), jnp.float32)
    D[0:TOP] = zeros
    for it in range(ITERS):
        for i in range(3):
            T[it, i, 0:TOP] = zeros
            A[it, i, 0:TOP] = zeros

    def blocks(low, high, size, body, init=0):
        return lax.fori_loop(
            0, (high - low) // size, lambda i, carry: body(low + i * size, carry), init
        )

    def each_row(stage, comps, count, store, first=0):
        def body(r, carry):
            for comp in range(comps):
                for j in range(8):
                    line = jnp.where(flip, (count - 8 - r) * 8 + 7 - j, r * 8 + j)
                    value = stage[pl.ds(comp * count * 8 + line, 8, stride=8), :]
                    store(comp, first + r + j, value)
            return carry

        blocks(0, count, 8, body)

    def store_x(comp, r, value):
        if comp == 1:
            value = value * sign
        X[comp, r] = value
        T[0, comp, TOP + r] = value

    @pl.when(own)
    def _():
        each_row(x_own, 3, rows, store_x)

    @pl.when(jnp.logical_not(own))
    def _():
        each_row(x_got, 3, part, store_x)

    pl.semaphore_wait(barrier, 2 * bands - 1 + far.astype(jnp.int32))

    def remote(src, dst, send, recv, to):
        return pltpu.make_async_remote_copy(
            src_ref=src, dst_ref=dst, send_sem=send, recv_sem=recv, device_id=to, device_id_type=MESH
        )

    rest_line = pl.multiple_of(jnp.where(flip, part * 8, 0), 128)
    rests = [
        remote(
            x_own.at[pl.ds(comp * rows * 8 + rest_line, rest * 8)],
            stg_r.at[pl.ds(comp * rest * 8, rest * 8)],
            rest_send.at[comp], rest_recv.at[comp], swap,
        )
        for comp in range(3)
    ]

    @pl.when(jnp.logical_not(own))
    def _():
        for copy in rests:
            copy.start()

    push_e = remote(e_own, stg_e, push_send.at[0], push_recv.at[0], partner)
    push_d = remote(d_own, stg_d, push_send.at[1], push_recv.at[1], partner)
    push_s = remote(s_own, stg_s, push_send.at[2], push_recv.at[2], partner)

    push_bottom = remote(d_own.at[edge_lines], d_bottom, push_send.at[3], push_recv.at[3], partner)
    push_top = [
        remote(
            d_own.at[edge_lines], d_top, push_send.at[4 + i], push_recv.at[4], (top_peer[0], 2 * (top_band // 2) + i)
        )
        for i in range(2)
    ]

    @pl.when(own)
    def _():
        push_d.start()
        pl.when(has_top)(lambda: [push.start() for push in push_top] and None)

    @pl.when(jnp.logical_not(own))
    def _():
        push_bottom.start()

    @pl.when(push_start)
    def _():
        push_s.start()

    def piece(ref, low, high, top):
        return ref.at[:, pl.ds(top + low, high - low)]

    def span(ends, j):
        return (ends[j - 1] if j else 0), ends[j]

    def x_copy(it, i):
        low, high = pieces[it][i]
        return remote(
            piece(X, low, high, 0), piece(XN.at[it], low, high, 0), x_send.at[it, i], x_recv.at[it, i], pred
        )

    arrived, sent, late = set(), set(), {}

    def some(done, it, low, high):
        fresh = [i for i, (p, q) in enumerate(pieces[it]) if p < high and q > low and (it, i) not in done]
        done.update((it, i) for i in fresh)
        return fresh

    def need_x(it, low, high):
        fresh = some(arrived, it, low, high)

        @pl.when(not_last)
        def _():
            for i in fresh:
                x_copy(it, i).wait_recv()

    def need_sent(it, low, high):
        fresh = some(sent, it, low, high)

        @pl.when(not_first)
        def _():
            for i in fresh:
                x_copy(it, i).wait_send()

    def send_x(it, low, high, late=None):
        @pl.when(not_first)
        def _():
            for i, (p, q) in enumerate(pieces[it]):
                if p >= low and q <= high and (late is None or late == (q > part)):
                    x_copy(it, i).start()

    def e_copy(it, j):
        low, high = span(plan[it][1], j)
        return remote(
            piece(T.at[it], low, high, TOP), piece(EN.at[it], low, high, 0),
            e_send.at[it, j], e_recv.at[it, j], succ,
        )

    def fin_copy(j):
        low, high = span(plan[-1][3], j)
        return remote(piece(X, low, high, 0), piece(FIN, low, high, 0), fin_send.at[j], fin_recv.at[j], swap)

    def halo_copy(h, side):
        return remote(
            edge_out.at[h, side], edge_in.at[h, side], halo_send.at[h, side], halo_recv.at[h, side],
            bottom_peer if side else top_peer,
        )

    def send_halo(h, side, get):
        def pack():
            for comp in range(3):
                for i in range(HALO):
                    value = get(comp, rows - 1 - i if side else i)
                    edge_out[h, side, comp, i if side else HALO - 1 - i] = -value if comp == 1 else value
            halo_copy(h, side).start()

        if side:
            pack()
        else:
            pl.when(has_top)(pack)

    def take_halo(h, side, buf):
        def unpack():
            halo_copy(h, side).wait()
            at = TOP + rows if side else TOP - HALO
            for comp in range(3):
                buf[comp, at : at + HALO] = edge_in[h, side, comp]

        if side:
            unpack()
        else:
            pl.when(has_top)(unpack)

    send_x(0, 0, part, False)
    send_halo(0, 0, lambda comp, r: X[comp, r])

    def send_late():
        send_x(0, 0, rows, True)
        send_halo(0, 1, lambda comp, r: X[comp, r])

    pl.when(own)(send_late)

    @pl.when(own)
    def _():
        push_e.start()

    def store_d(comp, r, value):
        D[TOP + r] = HALF * value

    @pl.when(own)
    def _():
        each_row(d_own, 1, rows, store_d)

    @pl.when(jnp.logical_not(own))
    def _():
        push_d.wait_recv()
        each_row(stg_d, 1, rows, store_d)


    def edge_line(i, mirrored, line=0):
        plain, back = i // 8 * 64 + i % 8, (15 - i) // 8 * 64 + (15 - i) % 8
        return pl.ds(line + jnp.where(mirrored, back, plain), 8, stride=8)

    def take_bottom(ref, line):
        for i in range(HALO):
            D[TOP + rows + i] = HALF * ref[edge_line(i, flip, line), :]

    @pl.when(own)
    def _():
        push_bottom.wait_recv()
        take_bottom(d_bottom, 0)

    @pl.when(jnp.logical_not(own))
    def _():
        take_bottom(d_own, jnp.where(flip, rows * 8 - 128, 0))

    @pl.when(has_top)
    def _():
        push_top[0].wait_recv()
        for i in range(HALO):
            D[TOP - 1 - i] = HALF * d_top[edge_line(i, jnp.logical_not(flip)), :]

    def run_forward(it, j):
        ends = plan[it][0]
        n = len(ends)
        if j == 0:
            take_halo(2 * it, 0, T.at[it])
        if j == n - 1:
            take_halo(2 * it, 1, T.at[it])
        low = TOP + ends[j - 1] if j else TOP - HALO + 2
        forward(T.at[it], D, F, low, TOP + ends[j], None if j else edge)
        pl.when(not_last)(lambda: e_copy(it, j).start())

    def send_edge(it, side):
        if side:
            need_x(it, rows - HALO, rows)
        else:
            early = some(arrived, it, 0, HALO)
            pl.when(not_last & has_top)(lambda: [x_copy(it, i).wait_recv() for i in early] and None)
            late[it] = early

        def get(comp, r):
            value = E[comp, r] * (XN[it, comp, r] - T[it, comp, TOP + r])
            return jnp.where(not_last, value, 0.0)

        send_halo(2 * it + 1, side, get)

    def run_adjoint(it, j):
        ends = plan[it][1]
        n = len(ends)
        low, high = span(ends, j)
        need_x(it, low, high)
        if j == 0:
            top_free = jnp.logical_not(has_top)
            pl.when(not_last & top_free)(lambda: [x_copy(it, i).wait_recv() for i in late[it]] and None)

        def differ(r, carry):
            at, wide = pl.ds(r, 4), pl.ds(TOP + r, 4)
            for comp in range(3):
                value = E[comp, at] * (XN[it, comp, at] - T[it, comp, wide])
                A[it, comp, wide] = jnp.where(not_last, value, 0.0)
            return carry

        blocks(low, high, 4, differ)
        if j == 0:
            take_halo(2 * it + 1, 0, A.at[it])
        if j == n - 1:
            take_halo(2 * it + 1, 1, A.at[it])
        low = TOP + low if j else TOP - HALO + 2
        adjoint(A.at[it], D, F, low, TOP + plan[it][2][j], None if j else edge)

    def run_update(it, j, acc):
        ends = plan[it][3]
        n = len(ends)
        final = it == ITERS - 1
        low, high = span(ends, j)

        @pl.when(not_first)
        def _():
            e_copy(it, j).wait_recv()

        need_sent(it, low, high)

        def update(r, acc):
            at, wide = pl.ds(r, 4), pl.ds(TOP + r, 4)
            for comp in range(3):
                x = X[comp, at]
                gap = x - EN[it, comp, at]
                lam = E[comp, at] * gap
                wy = WY[comp, at]
                grad = W[comp, at] * x - wy
                acc = acc + 0.5 * jnp.sum(lam * gap + x * (grad - wy), axis=0)
                x = x - STEP_SIZE * (lam - A[it, comp, wide] + grad)
                X[comp, at] = x
                if not final:
                    T[it + 1, comp, wide] = x
            return acc

        if high > low:
            acc = blocks(low, high, 4, update, acc)
            if final:
                pl.when(jnp.logical_not(own))(lambda: fin_copy(j).start())
            else:
                send_x(it + 1, low, high)
        if not final and j == 0:
            send_halo(2 * it + 2, 0, lambda comp, r: X[comp, r])
        if not final and j == n - 1:
            send_halo(2 * it + 2, 1, lambda comp, r: X[comp, r])
        return acc

    def take_rest():
        for copy in rests:
            copy.wait()
        each_row(stg_r, 3, rest, store_x, part)
        send_late()

    for j, high in enumerate(plan[0][0]):
        if j and plan[0][0][j - 1] == part:
            pl.when(jnp.logical_not(own))(take_rest)
        if high < rows:
            run_forward(0, j)

    @pl.when(own)
    def _():
        push_d.wait_send()
        push_e.wait_send()
        pl.when(has_top)(lambda: [push.wait_send() for push in push_top] and None)

    @pl.when(jnp.logical_not(own))
    def _():
        push_e.wait_recv()
        push_bottom.wait_send()

    def store_e(comp, r, value):
        E[comp, r] = value

    pl.when(own)(lambda: each_row(e_own, 3, rows, store_e))
    pl.when(jnp.logical_not(own))(lambda: each_row(stg_e, 3, rows, store_e))
    send_edge(0, 0)
    run_forward(0, len(plan[0][0]) - 1)
    send_edge(0, 1)

    pl.when(push_start)(lambda: push_s.wait_send())
    pl.when(need_start)(lambda: push_s.wait_recv())

    def store_s(comp, r, value):
        if comp == 1:
            value = value * sign
        EN[0, comp, r] = value
        EN[1, comp, r] = value

    pl.when(own_start)(lambda: each_row(s_own, 3, rows, store_s))
    pl.when(need_start)(lambda: each_row(stg_s, 3, rows, store_s))

    acc = [0.5 * c0_ref[...] for _ in range(ITERS)]
    for token in SCHEDULE:
        kind, it, j = token[0], int(token[1]), int(token[2])
        if kind == "F":
            run_forward(it, j)
        elif kind == "E":
            send_edge(it, j)
        elif kind == "A":
            run_adjoint(it, j)
        else:
            acc[it] = run_update(it, j, acc[it])
    for it in range(ITERS):
        cbuf[it] = acc[it]

    def c_copy(s):
        return remote(cbuf, crecv.at[band], c_send.at[s], c_recv.at[band], (2 * y + c, s))

    for s in range(bands):

        @pl.when(jnp.logical_not(own & (sp == s)))
        def _(s=s):
            c_copy(s).start()

    @pl.when(own)
    def _():
        crecv[band] = cbuf[...]

    flip_out = c == 1

    sign_out = jnp.where(flip_out, -1.0, 1.0).astype(jnp.float32)

    def put(src, j):
        low, high = span(plan[-1][3], j)

        def body(r, carry):
            for comp in range(3):
                for i in range(8):
                    value = src[comp, r + i]
                    line = jnp.where(flip_out, (rows - 8 - r) * 8 + 7 - i, r * 8 + i)
                    at = pl.ds(comp * rows * 8 + line, 8, stride=8)
                    OUT[at, :] = value * sign_out if comp == 1 else value
            return carry

        blocks(low, high, 8, body)

    used = [j for j in range(len(plan[-1][3])) if span(plan[-1][3], j)[1] > span(plan[-1][3], j)[0]]
    for j in used:

        @pl.when(own)
        def _():
            put(X, j)

        @pl.when(jnp.logical_not(own))
        def _():
            fin_copy(j).wait_recv()
            put(FIN, j)

    for s in range(bands):

        @pl.when(jnp.logical_not(own & (sp == s)))
        def _(s=s):
            c_copy(s).wait_send()

        @pl.when(jnp.logical_not(own & (band == s)))
        def _(s=s):
            remote(cbuf, crecv.at[s], c_send.at[s], c_recv.at[s], partner).wait_recv()

    total = crecv[0]
    for s in range(1, bands):
        total = total + crecv[s]
    for it in range(ITERS):
        cost_ref[0, it] = jnp.sum(total[it]) / cells

    @pl.when(not_last)
    def _():
        for it in range(ITERS):
            for j in range(len(plan[it][1])):
                e_copy(it, j).wait_send()

    @pl.when(jnp.logical_not(own))
    def _():
        for j in used:
            fin_copy(j).wait_send()


def as_tiles(x):
    x = x.reshape(-1, 8, x.shape[-1] // 128, 128)
    return x.transpose(0, 2, 1, 3).reshape(-1, 128)


def from_tiles(x, shape):
    x = x.reshape(-1, shape[-1] // 128, 8, 128)
    return x.transpose(0, 2, 1, 3).reshape(shape)


def per_device(
    increments, start_state, depth, error_weight, obs_index, obs_count, obs_value, obs_weight
):
    rows, columns = increments.shape[2:]
    slots = obs_index.shape[1]
    bands, windows = lax.axis_size("space"), lax.axis_size("tm")
    pairs = windows // 2
    total_rows = rows * bands
    cells = 3 * total_rows * columns
    _, _, a, y, b, c, band, _ = place()
    own = a == c

    exchange = []
    for py in range(pairs):
        for pb in range(bands // 2):
            one = 2 * py * bands + 2 * pb + 1
            two = (2 * py + 1) * bands + 2 * pb
            exchange += [(one, two), (two, one)]
    both = ("tm", "space")

    live = jnp.arange(slots) < obs_count[0]
    packed = jnp.stack(
        [obs_index[0].astype(jnp.float32), jnp.where(live, obs_weight[0], 0.0), obs_value[0]]
    )
    packed = lax.optimization_barrier(packed)
    packed_got = lax.ppermute(packed, both, exchange)
    early = early_rows(rows)
    x_early = jnp.where(a == 1, increments[:, :, :early], increments[:, :, rows - early :])
    x_got = lax.ppermute(x_early, both, exchange)
    packed = jnp.where(own, packed, packed_got)

    index = packed[0].astype(jnp.int32)
    component = index // (total_rows * columns)
    line = index // columns % total_rows - band * rows
    inside = (line >= 0) & (line < rows)
    flip = a == 1
    line = jnp.where(flip, rows - 1 - line, line)
    code = (component * rows + jnp.clip(line, 0, rows - 1)) * columns + index % columns
    weight = jnp.where(inside, packed[1], 0.0)
    weighted = weight * packed[2]
    c0 = jnp.sum((weighted * packed[2]).reshape(-1, 8, 128), 0)
    weighted = jnp.where(flip & (component == 1), -weighted, weighted)

    wide = rows + 2 * TOP
    line = jnp.arange(wide) - TOP
    line = band * rows + jnp.where(flip, rows - 1 - line, line)
    latitude = (line.astype(jnp.float32) + 0.5) / total_rows
    rate = CORIOLIS_MAX * jnp.sin(latitude * math.pi - math.pi / 2)
    rate = jnp.where(flip, -rate, rate)
    rate = jnp.broadcast_to(rate[:, None, None], (wide, 8, 128))
    code, weight, weighted, rate, c0 = lax.optimization_barrier((code, weight, weighted, rate, c0))

    lines = 3 * rows * 8
    smem = pl.BlockSpec(memory_space=pltpu.SMEM)
    vmem = pl.BlockSpec(memory_space=pltpu.VMEM)
    grid_type = jax.ShapeDtypeStruct((lines, 128), jnp.float32)
    grid_w, grid_wy = pl.pallas_call(
        functools.partial(deposit_kernel, slots),
        out_shape=(grid_type, grid_type),
        in_specs=[smem] * 3,
        out_specs=(vmem, vmem),
        scratch_shapes=[pltpu.VMEM((lines, 128), jnp.float32)] * (2 * STREAMS - 2),
        compiler_params=pltpu.CompilerParams(vmem_limit_bytes=16 * 2**20),
        cost_estimate=pl.CostEstimate(flops=10**10, bytes_accessed=10**8, transcendentals=0),
        name="deposit",
    )(code, weight, weighted)

    def rows_of(count, lead=(3,)):
        return pltpu.VMEM((*lead, count, 8, 128), jnp.float32)

    tiles = pltpu.VMEM((lines, 128), jnp.float32)
    dma = pltpu.SemaphoreType.DMA
    chunks = len(limits(rows)[-1][0])
    sends = max(map(len, sent_pieces(rows)))
    halo = (HALO, 8, 128)
    out, costs = pl.pallas_call(
        functools.partial(main_kernel, rows, cells, pairs, bands),
        out_shape=(grid_type, jax.ShapeDtypeStruct((1, ITERS), jnp.float32)),
        in_specs=[vmem] * 9,
        out_specs=(vmem, smem),
        scratch_shapes=[
            pltpu.VMEM((3 * (rows - early) * 8, 128), jnp.float32),
            tiles, pltpu.VMEM((rows * 8, 128), jnp.float32), tiles,
            rows_of(rows), rows_of(wide, (ITERS, 3)), rows_of(wide, (ITERS, 3)),
            rows_of(wide, ()), rows_of(rows),
            rows_of(rows, (ITERS, 3)), rows_of(rows, (ITERS, 3)), rows_of(rows),
            pltpu.VMEM((ITERS, 8, 128), jnp.float32), pltpu.VMEM((bands, ITERS, 8, 128), jnp.float32),
            pltpu.VMEM((2 * ITERS, 2, 3, *halo), jnp.float32), pltpu.VMEM((2 * ITERS, 2, 3, *halo), jnp.float32),
            pltpu.VMEM((128, 128), jnp.float32), pltpu.VMEM((128, 128), jnp.float32),
            dma((6,)), dma((5,)), dma((3,)), dma((3,)), dma((2 * ITERS, 2)), dma((2 * ITERS, 2)),
            dma((ITERS, sends)), dma((ITERS, sends)), dma((ITERS, chunks)), dma((ITERS, chunks)),
            dma((chunks,)), dma((chunks,)), dma((bands,)), dma((bands,)),
        ],
        compiler_params=pltpu.CompilerParams(
            collective_id=0, has_side_effects=True, vmem_limit_bytes=VMEM * 2**20
        ),
        name="iterations",
    )(
        as_tiles(increments), as_tiles(x_got), as_tiles(error_weight), as_tiles(depth),
        as_tiles(start_state), grid_w.reshape(3, rows, 8, 128), grid_wy.reshape(3, rows, 8, 128),
        rate, c0,
    )
    return from_tiles(out, increments.shape), costs.T


def solution(mesh):
    placed = (
        P("tm", None, "space", None),
        P(None, "space", None),
        P("space", None),
        P(None, "space", None),
        P("tm", None),
        P("tm"),
        P("tm", None),
        P("tm", None),
    )
    return jax.shard_map(
        per_device,
        mesh=mesh,
        in_specs=placed,
        out_specs=(P("tm", None, "space", None), P(None, "tm")),
        check_vma=False,
    )
```
